32 devices in a mesh: seq: 8 (over z, core), vocab: 4 (over y, x).
Axes of the slice: x: 2, y: 2, z: 4, core: 2. Of those that a mesh axis runs over, the one named last changes fastest.
Arguments:
- token_ids: int32 [1024], P('seq'), may hold values from 0 to 76031, as said below
- routes: int32 [256, 1], P('seq'), may hold values from 0 to 7; in each aligned block of 32 rows (0 to 31, 32 to 63, ...) at most 8 rows name the same one
- splice_start: int32 [8], P('seq'), may hold values from 0 to 64
- vision: bfloat16 [256, 5120], P('seq'), may hold values from -6 to 6
- ln_gain: float32 [1280], replicated, may hold values from 0.25 to 1.75
- table: bfloat16 [76032, 8192], P('seq', 'vocab'), may hold values from -6 to 6
- w_fc1: bfloat16 [5120, 5120], P('seq', 'vocab'), may hold values from -0.078125 to 0.078125
- w_fc2: bfloat16 [5120, 8192], P('seq', 'vocab'), may hold values from -0.078125 to 0.078125
Outputs:
- embedded: bfloat16 [1024, 8192], P('seq', 'vocab')
The draws below stay inside these ranges and needn't reach their ends.
Inputs may be any that keep to these rules, and one draw needn't show every extreme that they name: `routes`: among the rows of one shard of 32 rows no sequence is named by more than 8 rows. `token_ids`: split the vocabulary into 8 equal ranges of consecutive ids; within one sequence of 128 tokens at most 32 ids fall in one range, and every sequence has a range with exactly 32.
All inputs are finite; a program needn't handle non-finite values.
Results may differ from the reference program's by a relative error of at most 0.0055.
Values may be sent and summed in bfloat16 or wider, within the bound.
A program may use at most 128 MiB of HBM per device.

```python
import math
import jax
import jax.numpy as jnp
import numpy as np
from jax import lax

D = 8192
VIS = 1280
VOCAB = 76032
TOK_OWN = 128
MERGE = 5120
SLOTS = 32
PAIR_CAP = 8
ROWS_ALL = 256
N_SEQ = 8


def draw_token_ids(key, part):
    id_cap = 2 * TOK_OWN // N_SEQ
    shard_rows = VOCAB // N_SEQ
    half = TOK_OWN // 2
    heavy = 3 * id_cap // 4

    def one_sequence(seq_key):
        key_hot, key_order, key_offset = jax.random.split(seq_key, 3)
        hot = jax.random.randint(key_hot, (), 0, N_SEQ).astype(jnp.int32)
        places = jnp.arange(TOK_OWN, dtype=jnp.int32)
        others = places - half - heavy
        second = jnp.where(places - half < heavy, hot, (hot + 1 + others % (N_SEQ - 1)) % N_SEQ)
        labels = jnp.where(places < half, places % N_SEQ, second).astype(jnp.int32)
        labels = jax.random.permutation(key_order, labels)
        offsets = jax.random.randint(key_offset, (TOK_OWN,), 0, shard_rows).astype(jnp.int32)
        return (labels * shard_rows + offsets).astype(jnp.int32)
    keys = jax.random.split(jax.random.fold_in(key, 7), N_SEQ)
    return jax.vmap(one_sequence)(keys).reshape(N_SEQ * TOK_OWN).astype(jnp.int32)


def with_ends(array, rng, smallest, largest):
    place = [jax.random.randint(jax.random.fold_in(rng, axis), (), 0, length) for axis, length in enumerate(array.shape)]
    longest = array.shape.index(max(array.shape))
    beside = place[:longest] + [(place[longest] + 1) % array.shape[longest]] + place[longest + 1:]
    return array.at[tuple(place)].set(smallest).at[tuple(beside)].set(largest)


def block_scale(stream_key, dims, cuts, low, high):
    def one(dim, blocks):
        heights = jax.random.uniform(jax.random.fold_in(jax.random.fold_in(stream_key, 6), dim), (blocks,), jnp.float32, low / len(cuts), high / len(cuts))
        return jnp.repeat(jnp.exp(heights), dims[dim] // blocks).reshape((-1,) + (1,) * (len(dims) - dim - 1))

    level = one(*cuts[0])
    for cut in cuts[1:]:
        level = level * one(*cut)
    return level


def shared_out(own_key, own, number, rows, count, top, most, lean):
    sequence = jax.random.permutation(own_key, count)
    heavy_load, ordinary = portions_of(count, rows * top, most, lean, True), portions_of(count, rows * top, most, lean, False)
    places = jnp.arange(count)

    def named(sizes, offset_by):
        used = int((sizes > 0).sum())
        fixed = max(1, used // 4)
        shifted = fixed + (places - fixed + offset_by * (used - fixed)) % max(1, count - fixed)
        return jnp.zeros((count,), jnp.int32).at[sequence[jnp.where(places < fixed, places, shifted)]].set(jnp.asarray(sizes, jnp.int32))

    sizes = jnp.where(number % 4 == 0, named(heavy_load, number // 4), named(ordinary, number - number // 4 - 1))
    mixed = jax.random.permutation(jax.random.fold_in(own, 3), count)
    source_of, receiver = mixed[0:count // 2 * 2:2], mixed[1:count // 2 * 2:2]
    margin = jnp.minimum(sizes[source_of] - 1, most - sizes[receiver]) // 2
    margin = jnp.where((source_of == sequence[0]) | (receiver == sequence[0]) | (sizes[receiver] == 0), 0, jnp.maximum(margin, 0))
    shifted = jax.random.randint(jax.random.fold_in(own, 4), (count // 2,), 0, 1 << 20) % (margin + 1)
    sizes = sizes.at[source_of].add(-shifted).at[receiver].add(shifted)
    items = jnp.searchsorted(jnp.cumsum(sizes), jnp.arange(rows * top), side="right").astype(jnp.int32)
    table = items.reshape(top, rows).T
    table = table[jax.random.permutation(jax.random.fold_in(own, 1), rows)]
    offset_by = jax.random.randint(jax.random.fold_in(own, 2), (rows, 1), 0, top)
    return jnp.take_along_axis(table, (jnp.arange(top)[None, :] + offset_by) % top, axis=1)


def portions_of(number_of, total, most, skew, full):
    weights = [(1 << 20) // math.isqrt(grade ** skew) + 1 for grade in range(1, number_of + 1)]
    largest = most if full else min(most, max(-(-total // number_of), total * weights[0] // sum(weights)))
    least = 1 if total - largest >= number_of - 1 else 0
    counts, rest = [largest] + [least] * (number_of - 1), total - largest - least * (number_of - 1)
    while rest > 0:
        movable = [i for i in range(1, number_of) if counts[i] < largest] or [i for i in range(1, number_of) if counts[i] < most]
        pool, left = sum([weights[i] for i in movable]), rest
        for i in movable:
            addition = min(most - counts[i], max(1, left * weights[i] // pool), rest)
            counts[i] = counts[i] + addition
            rest = rest - addition
    return np.array(counts)


def noise(key, dims, width, bound, shards=(), held_as=jnp.bfloat16):
    array = width * jax.random.normal(key, dims, jnp.float32)
    if shards:
        array = array * block_scale(key, dims, shards, -0.22, 0.18)
    return jnp.clip(array, -bound, bound).astype(held_as)


def setup_inputs(seed: int = 0) -> dict:
    seeds = jax.random.split(jax.random.key(seed), 9)
    token_ids = draw_token_ids(jax.random.fold_in(seeds[8], 71), 0)
    routes_keys = jax.random.split(jax.random.fold_in(seeds[1], 1), ROWS_ALL // SLOTS)
    routes_turns = jax.random.permutation(jax.random.fold_in(seeds[1], 3), ROWS_ALL // SLOTS)
    routes = jax.vmap(lambda own, number: shared_out(jax.random.fold_in(seeds[1], 2), own, number, SLOTS, N_SEQ, 1, PAIR_CAP, 2))(routes_keys, routes_turns).reshape((ROWS_ALL, 1))
    splice_start = with_ends(jax.random.randint(seeds[2], (N_SEQ,), 0, TOK_OWN - 2 * SLOTS + 1), jax.random.fold_in(seeds[2], 1), 0, TOK_OWN - 2 * SLOTS).astype(jnp.int32)
    vision = noise(seeds[3], (ROWS_ALL, MERGE), 1.0, 6.0, ((0, 8),))
    ln_gain = jnp.clip(1.0 + 0.15 * jax.random.normal(seeds[4], (VIS,), jnp.float32), 0.25, 1.75)
    table = noise(seeds[5], (VOCAB, D), 1.0, 6.0, ((0, 8), (1, 4)))
    w_fc1 = noise(seeds[6], (MERGE, MERGE), MERGE ** -0.5, 0.078125, ((0, 8), (1, 4)))
    w_fc2 = noise(seeds[7], (MERGE, D), MERGE ** -0.5, 0.078125, ((0, 8), (1, 4)))
    return dict(token_ids=token_ids, routes=routes, splice_start=splice_start, vision=vision, ln_gain=ln_gain, table=table, w_fc1=w_fc1, w_fc2=w_fc2)


def layer_norm(vision, ln_gain):
    rows = vision.shape[0]
    values = vision.astype(jnp.float32).reshape(rows, 4, ln_gain.shape[0])
    center = values - lax.optimization_barrier(jnp.mean(values, axis=-1, keepdims=True))
    spread = lax.optimization_barrier(jnp.mean(center * center, axis=-1, keepdims=True))
    normed = center / jnp.sqrt(spread + 1e-06) * ln_gain.astype(jnp.float32)
    return normed.reshape(rows, 4 * ln_gain.shape[0]).astype(jnp.bfloat16)

def reference(token_ids, routes, splice_start, vision, ln_gain, table, w_fc1, w_fc2):
    text = jnp.take(table, token_ids.astype(jnp.int32), axis=0)
    normed = layer_norm(vision, ln_gain)
    pre = jnp.dot(normed, w_fc1, preferred_element_type=jnp.float32)
    hidden = jax.nn.gelu(pre, approximate=False).astype(jnp.bfloat16)
    merged = jnp.dot(hidden, w_fc2, preferred_element_type=jnp.float32).astype(jnp.bfloat16)
    owners = routes[:, 0].astype(jnp.int32)
    owner_hot = (owners[:, None] == jnp.arange(N_SEQ, dtype=jnp.int32)[None, :]).astype(jnp.int32)
    earlier = jnp.cumsum(owner_hot, axis=0) - owner_hot
    rank = lax.optimization_barrier(jnp.sum(earlier * owner_hot, axis=1)).astype(jnp.int32)
    target = (owners * TOK_OWN + jnp.take(splice_start, owners).astype(jnp.int32) + rank).astype(jnp.int32)
    return text.at[target].set(merged)
```

```python
import math

import jax
import jax.numpy as jnp
from jax import lax
from jax.experimental import pallas as pl
from jax.experimental.pallas import tpu as pltpu
from jax.sharding import PartitionSpec as P


TILE = 8


def gather_kernel(ids_ref, pick_ref, table_ref, out_ref, held, sems):
    groups, cap, _ = out_ref.shape

    def issue(g, carry):
        def one(k, c):
            row = pl.multiple_of(ids_ref[g, k] // TILE * TILE, TILE)
            at = pl.multiple_of((g * cap + k) * TILE, TILE)
            pltpu.make_async_copy(
                table_ref.at[pl.ds(row, TILE), :], held.at[pl.ds(at, TILE), :], sems.at[g]
            ).start()
            return c

        return lax.fori_loop(0, cap, one, carry)

    lax.fori_loop(0, groups, issue, 0)

    def finish(g, carry):
        at = pl.multiple_of(g * cap * TILE, TILE)
        block = held.at[pl.ds(at, cap * TILE), :]
        pltpu.make_async_copy(block, block, sems.at[g]).wait()
        out_ref[g] = jnp.dot(
            pick_ref[g], block[...], preferred_element_type=jnp.float32
        ).astype(out_ref.dtype)
        return carry

    lax.fori_loop(0, groups, finish, 0)


def gather_rows(local_ids, table):
    groups, cap = local_ids.shape
    width = table.shape[1]
    lane = jnp.arange(cap * TILE, dtype=jnp.int32)
    slot = jnp.arange(cap, dtype=jnp.int32)[None, :] * TILE + local_ids % TILE
    pick = (slot[:, :, None] == lane[None, None, :]).astype(jnp.bfloat16)
    return pl.pallas_call(
        gather_kernel,
        out_shape=jax.ShapeDtypeStruct((groups, cap, width), table.dtype),
        in_specs=[
            pl.BlockSpec(memory_space=pltpu.SMEM),
            pl.BlockSpec(memory_space=pltpu.VMEM),
            pl.BlockSpec(memory_space=pl.ANY),
        ],
        out_specs=pl.BlockSpec(memory_space=pltpu.VMEM),
        scratch_shapes=[
            pltpu.VMEM((groups * cap * TILE, width), table.dtype),
            pltpu.SemaphoreType.DMA((groups,)),
        ],
        name="gather_rows",
    )(local_ids, pick, table)


def route_plan(token_ids, routes, splice_start, shard_rows):
    seq_count = lax.axis_size("seq")
    seq_index = lax.axis_index("seq")
    local_rows = token_ids.shape[0]
    slot_rows = routes.shape[0]
    pair_cap = 2 * slot_rows // seq_count
    id_cap = 2 * local_rows // seq_count
    both = lax.all_gather(jnp.concatenate([token_ids, routes[:, 0]]), "seq", axis=0)
    all_ids, all_routes = both[:, :local_rows], both[:, local_rows:]
    mine = all_ids // shard_rows == seq_index
    place = jnp.cumsum(mine.astype(jnp.int32), axis=1) - 1
    hit = mine[:, None, :] & (
        place[:, None, :] == jnp.arange(id_cap, dtype=jnp.int32)[None, :, None]
    )
    local_ids = jnp.sum(jnp.where(hit, all_ids[:, None, :] - seq_index * shard_rows, 0), axis=2)
    home = token_ids // shard_rows
    same = (home[None, :] == home[:, None]) & (
        jnp.arange(local_rows)[None, :] < jnp.arange(local_rows)[:, None]
    )
    arrive = home * id_cap + jnp.sum(same.astype(jnp.int32), axis=1)
    own = routes[:, 0]
    earlier = (own[None, :] == own[:, None]) & (
        jnp.arange(slot_rows)[None, :] < jnp.arange(slot_rows)[:, None]
    )
    slot_of = own * pair_cap + jnp.sum(earlier.astype(jnp.int32), axis=1)
    selector = (
        slot_of[None, :] == jnp.arange(seq_count * pair_cap, dtype=jnp.int32)[:, None]
    ).astype(jnp.bfloat16)
    counts = jnp.sum((all_routes == seq_index).astype(jnp.int32), axis=1)
    before = jnp.arange(seq_count)[None, :] < jnp.arange(seq_count)[:, None]
    offset = jnp.sum(jnp.where(before, counts[None, :], 0), axis=1)
    within = jnp.arange(pair_cap, dtype=jnp.int32)
    position = jnp.where(
        within[None, :] < counts[:, None],
        splice_start[0] + offset[:, None] + within[None, :],
        -1,
    ).reshape(-1)
    rows = jnp.arange(local_rows, dtype=jnp.int32)
    image = position[None, :] == rows[:, None]
    first = splice_start[0]
    is_image = (rows >= first) & (rows < first + jnp.sum(counts))
    text = (
        arrive[:, None] == jnp.arange(seq_count * id_cap, dtype=jnp.int32)[None, :]
    ) & ~is_image[:, None]
    return local_ids, selector, image.astype(jnp.bfloat16), text.astype(jnp.bfloat16)


def mega_kernel(
    vision_ref, gain_ref, w1_hbm, w2_hbm, text_ref, selector_ref, image_ref, placed_ref, out_ref,
    w1, w2, x_send, x_recv, half_send, half_recv, half_own, plane_send, plane_recv, cross_recv,
    h_own, h_recv, pair_send, pair_recv, pair_own, part_send, part_recv,
    row_send, row_recv, text_recv, total,
    w_sem, x_sems, half_sems, plane_sems, cross_sems, h_sems,
    pair_sems, part_sems, row_sems, text_sems,
):
    n, voc = lax.axis_size("seq"), lax.axis_size("vocab")
    s, v = lax.axis_index("seq"), lax.axis_index("vocab")
    chips = n // 2
    z, c = s // 2, s % 2
    split = n // voc
    f32, bf16 = jnp.float32, jnp.bfloat16
    slots = vision_ref.shape[0]
    blocks, block = x_send.shape[1], x_send.shape[2]

    def at(seq, vocab):
        return dict(device_id=(seq, vocab), device_id_type=pl.DeviceIdType.MESH)

    load1 = pltpu.make_async_copy(w1_hbm, w1, w_sem.at[0])
    load2 = pltpu.make_async_copy(w2_hbm, w2, w_sem.at[1])
    load1.start()
    load2.start()

    barrier = pltpu.get_barrier_semaphore()
    for d in range(1, n):
        pl.semaphore_signal(barrier, inc=1, **at(lax.rem(s + d, n), v))
    for e in range(1, voc):
        pl.semaphore_signal(barrier, inc=1, **at(s, lax.rem(v + e, voc)))

    group = gain_ref.shape[1]
    depth = x_send.shape[3]
    for g in range(vision_ref.shape[1] // group):
        values = vision_ref[:, g * group : (g + 1) * group].astype(f32)
        center = values - jnp.mean(values, axis=-1, keepdims=True)
        spread = jnp.mean(center * center, axis=-1, keepdims=True)
        normed = (center / jnp.sqrt(spread + 1e-06) * gain_ref[...]).astype(bf16)
        for k in range(group // depth):
            part = normed[:, k * depth : (k + 1) * depth]
            for i in range(blocks):
                x_send[g * (group // depth) + k, i] = part[i * block : (i + 1) * block]

    pl.semaphore_wait(barrier, n - 1 + voc - 1)

    def to_peer(source, target, sems, d, seq, vocab=None):
        copy = pltpu.make_async_remote_copy(
            src_ref=source,
            dst_ref=target,
            send_sem=sems.at[0, d],
            recv_sem=sems.at[1, d],
            **at(seq, v if vocab is None else vocab),
        )
        copy.start()
        return copy

    def x_place(seq):
        if blocks == 1:
            return x_recv.at[pl.ds(seq % 2, 1), seq // 2]
        return x_recv.at[:, seq]

    copies = []
    for d in range(1, n):
        peer = lax.rem(s + d, n)
        copies.append(to_peer(x_send.at[peer], x_place(s), x_sems, d, peer))
    x_place(s)[...] = x_send[s]

    texts = []

    def send_text(ds):
        for d in ds:
            peer = lax.rem(s + d, n)
            texts.append(to_peer(text_ref.at[peer], text_recv.at[s], text_sems, d, peer))

    send_text(TEXT_A(n))
    text_recv[s] = text_ref[s]
    for copy in copies:
        copy.wait()

    def columns(width):
        return 256 if width % 256 == 0 else width

    def chip_sums(lhs_ref, weight, to_sib, from_sib, own, sems_pair):
        width = weight.shape[1]
        step = columns(width)
        for core, keep in ((1 - c, False), (c, True)):
            lhs = lhs_ref[core].reshape(-1, weight.shape[0])
            for k in range(0, width, step):
                part = jnp.dot(lhs, weight[:, k : k + step], preferred_element_type=f32)
                if keep:
                    own[:, k : k + step] = part
                else:
                    to_sib[:, k : k + step] = part.astype(bf16)
            if not keep:
                swap = to_peer(to_sib, from_sib, sems_pair, 0, s + 1 - 2 * c)
        swap.wait()

    load1.wait()
    chip_sums(x_recv, w1, half_send, half_recv, half_own, half_sems)
    copies = []
    for e in range(1, voc):
        peer = lax.rem(v + e, voc)
        span = pl.ds(pl.multiple_of(peer * block, block), block)
        plane_send[e] = (half_own[span, :] + half_recv[span, :].astype(f32)).astype(bf16)
        copies.append(to_peer(plane_send.at[e], plane_recv.at[v], plane_sems, e, s, peer))
    send_text(TEXT_B(n))
    span = pl.ds(pl.multiple_of(v * block, block), block)
    plane_recv[v] = (half_own[span, :] + half_recv[span, :].astype(f32)).astype(bf16)
    for copy in copies:
        copy.wait()

    inner = h_own.shape[2]

    def hidden_part(seq):
        side = pl.multiple_of(seq % split * inner, inner) if split > 1 else 0
        return plane_recv.at[seq // split, :, pl.ds(side, inner)]

    copies = []
    for d in range(1, n):
        peer = lax.rem(s + d, n)
        copies.append(to_peer(hidden_part(peer), cross_recv.at[s], cross_sems, d, peer))
    cross_recv[s] = hidden_part(s)[...]
    send_text(TEXT_C(n))
    for copy in copies:
        copy.wait()
    for core in range(2):
        pre = cross_recv[core].astype(f32)
        for k in range(1, chips):
            pre = pre + cross_recv[2 * k + core].astype(f32)
        h_own[core] = (0.5 * pre * (1.0 + lax.erf(pre * math.sqrt(0.5)))).astype(bf16)

    def h_place(vocab):
        if blocks == 1:
            return h_recv.at[:, vocab, 0]
        return h_recv.at[vocab % 2, vocab // 2]

    copies = []
    for e in range(1, voc):
        peer = lax.rem(v + e, voc)
        copies.append(to_peer(h_own, h_place(v), h_sems, e, s, peer))
    h_place(v)[...] = h_own[...]
    load2.wait()
    for copy in copies:
        copy.wait()

    width = w2.shape[1]
    chip_sums(h_recv, w2, pair_send, pair_recv, pair_own, pair_sems)
    sent = []
    for d in range(1, chips):
        other = lax.rem(z + d, chips)
        span = pl.ds(pl.multiple_of(other * slots, slots), slots)
        part_send[d] = (pair_own[span, :] + pair_recv[span, :].astype(f32)).astype(bf16)
        sent.append(to_peer(part_send.at[d], part_recv.at[d], part_sems, d, other * 2 + c))
    send_text(TEXT_D(n))
    span = pl.ds(pl.multiple_of(z * slots, slots), slots)
    value = pair_own[span, :] + pair_recv[span, :].astype(f32)
    for copy in sent:
        copy.wait()
    for d in range(1, chips):
        value = value + part_recv[d].astype(f32)
    merged = value.astype(bf16)

    cap = row_send.shape[1]
    outgoing = jnp.dot(selector_ref[...], merged, preferred_element_type=f32).astype(bf16)
    for t in range(n):
        row_send[t] = outgoing[t * cap : (t + 1) * cap]
    copies = []
    for d in range(1, n):
        peer = lax.rem(s + d, n)
        copies.append(to_peer(row_send.at[peer], row_recv.at[s], row_sems, d, peer))
    row_recv[s] = row_send[s]
    for copy in texts:
        copy.wait()
    step = columns(width)
    found = text_recv[...].reshape(-1, width)
    for k in range(0, width, step):
        total[:, k : k + step] = jnp.dot(
            placed_ref[...], found[:, k : k + step], preferred_element_type=f32
        )
    for copy in copies:
        copy.wait()
    for k in range(0, width, step):
        value = total[:, k : k + step]
        block_rows = row_recv[:, :, k : k + step].astype(f32).reshape(n * cap, step).astype(bf16)
        value = value + jnp.dot(image_ref[...], block_rows, preferred_element_type=f32)
        out_ref[:, k : k + step] = value.astype(bf16)


def TEXT_A(n):
    return range(1, 2)


def TEXT_B(n):
    return range(2, n // 2)


def TEXT_C(n):
    return range(n // 2, 3 * n // 4)


def TEXT_D(n):
    return range(3 * n // 4, n)


def mega(vision, gain, w1, w2, text, selector, image_pick, text_pick):
    n, voc = lax.axis_size("seq"), lax.axis_size("vocab")
    slots = vision.shape[0]
    rows = n // 2 * slots
    block = n * slots // (2 * voc)
    blocks = slots // block
    depth, mid = w1.shape
    inner, width = w2.shape
    cap = selector.shape[0] // n
    bf16, f32 = jnp.bfloat16, jnp.float32
    vmem = pl.BlockSpec(memory_space=pltpu.VMEM)
    hbm = pl.BlockSpec(memory_space=pl.ANY)
    dma = pltpu.SemaphoreType.DMA
    return pl.pallas_call(
        mega_kernel,
        out_shape=jax.ShapeDtypeStruct((image_pick.shape[0], width), bf16),
        in_specs=[vmem, vmem, hbm, hbm, vmem, vmem, vmem, vmem],
        out_specs=vmem,
        scratch_shapes=[
            pltpu.VMEM(w1.shape, bf16),
            pltpu.VMEM(w2.shape, bf16),
            pltpu.VMEM((n, blocks, block, depth), bf16),
            pltpu.VMEM((2, voc, block, depth), bf16),
            pltpu.VMEM((voc * block, mid), bf16),
            pltpu.VMEM((voc * block, mid), bf16),
            pltpu.VMEM((voc * block, mid), f32),
            pltpu.VMEM((voc, block, mid), bf16),
            pltpu.VMEM((voc, block, mid), bf16),
            pltpu.VMEM((n, block, inner), bf16),
            pltpu.VMEM((2, block, inner), bf16),
            pltpu.VMEM((2, n // 2, blocks, block, inner), bf16),
            pltpu.VMEM((rows, width), bf16),
            pltpu.VMEM((rows, width), bf16),
            pltpu.VMEM((rows, width), f32),
            pltpu.VMEM((n // 2, slots, width), bf16),
            pltpu.VMEM((n // 2, slots, width), bf16),
            pltpu.VMEM((n, cap, width), bf16),
            pltpu.VMEM((n, cap, width), bf16),
            pltpu.VMEM(text.shape, bf16),
            pltpu.VMEM((image_pick.shape[0], width), f32),
            dma((2,)),
            dma((2, n)),
            dma((2, 1)),
            dma((2, voc)),
            dma((2, n)),
            dma((2, voc)),
            dma((2, 1)),
            dma((2, n // 2)),
            dma((2, n)),
            dma((2, n)),
        ],
        compiler_params=pltpu.CompilerParams(
            collective_id=0, has_side_effects=True, vmem_limit_bytes=40 * 1024 * 1024
        ),
        name="merger",
    )(vision, gain[None, :], w1, w2, text, selector, image_pick, text_pick)


def on_device(token_ids, routes, splice_start, vision, ln_gain, table, w_fc1, w_fc2):
    local_ids, selector, image_pick, text_pick = route_plan(
        token_ids, routes, splice_start, table.shape[0]
    )
    text = gather_rows(local_ids, table)
    return mega(vision, ln_gain, w_fc1, w_fc2, text, selector, image_pick, text_pick)


def solution(mesh):
    in_specs = (
        P("seq"),
        P("seq", None),
        P("seq"),
        P("seq", None),
        P(),
        P("seq", "vocab"),
        P("seq", "vocab"),
        P("seq", "vocab"),
    )
    out_specs = P("seq", "vocab")
    return jax.shard_map(
        on_device, mesh=mesh, in_specs=in_specs, out_specs=out_specs, check_vma=False
    )
```

```python
import math

import jax
import jax.numpy as jnp
from jax import lax
from jax.experimental import pallas as pl
from jax.experimental.pallas import tpu as pltpu
from jax.sharding import PartitionSpec as P


PAIR = 2
LANES = 128


def at(seq, vocab):
    return dict(device_id=(seq, vocab), device_id_type=pl.DeviceIdType.MESH)


def iota(shape, dim):
    return lax.broadcasted_iota(jnp.int32, shape, dim)


def x_slot(ref, seq, blocks):
    if blocks == 1:
        return ref.at[pl.ds(seq % 2, 1), seq // 2]
    return ref.at[:, seq]


def exchange_kernel(
    shard_rows, ids_ref, routes_ref, start_ref, vision_ref, gain_ref,
    local_ref, pick_ref, selector_ref, image_ref, placed_ref, x_ref,
    pack, pack_recv, x_send, x_recv, id_sems, x_sems,
):
    n = lax.axis_size("seq")
    s, v = lax.axis_index("seq"), lax.axis_index("vocab")
    f32, bf16, i32 = jnp.float32, jnp.bfloat16, jnp.int32
    tokens, slots = ids_ref.shape[1], routes_ref.shape[1]
    id_cap = local_ref.shape[1]
    cap = selector_ref.shape[0] // n
    blocks, block, depth = x_send.shape[1:]

    barrier = pltpu.get_barrier_semaphore()
    for d in range(1, n):
        pl.semaphore_signal(barrier, inc=1, **at(lax.rem(s + d, n), v))

    pack[...] = jnp.full(pack.shape, -1, i32)
    pack[0:1, :tokens] = ids_ref[...]
    pack[1:2, :slots] = routes_ref[...]
    pack_recv[s] = pack[...]

    group = gain_ref.shape[1]
    for g in range(vision_ref.shape[1] // group):
        values = vision_ref[:, g * group : (g + 1) * group].astype(f32)
        center = values - jnp.mean(values, axis=-1, keepdims=True)
        spread = jnp.mean(center * center, axis=-1, keepdims=True)
        normed = (center / jnp.sqrt(spread + 1e-06) * gain_ref[...]).astype(bf16)
        for k in range(group // depth):
            part = normed[:, k * depth : (k + 1) * depth]
            for i in range(blocks):
                x_send[g * (group // depth) + k, i] = part[i * block : (i + 1) * block]

    pl.semaphore_wait(barrier, n - 1)

    def to_peer(source, target, sems, d, seq):
        copy = pltpu.make_async_remote_copy(
            src_ref=source,
            dst_ref=target,
            send_sem=sems.at[0, d],
            recv_sem=sems.at[1, d],
            **at(seq, v),
        )
        copy.start()
        return copy

    id_copies, x_copies = [], []
    for d in range(1, n):
        peer = lax.rem(s + d, n)
        id_copies.append(to_peer(pack, pack_recv.at[s], id_sems, d, peer))
    for d in range(1, n):
        peer = lax.rem(s + d, n)
        x_copies.append(
            to_peer(x_send.at[peer], x_slot(x_recv, s, blocks), x_sems, d, peer)
        )
    x_slot(x_recv, s, blocks)[...] = x_send[s]

    lane_t = iota((tokens, tokens), 1)
    upto = (iota((tokens, tokens), 0) <= lane_t).astype(bf16)
    before = (iota((tokens, tokens), 0) < lane_t).astype(bf16)

    own = ids_ref[...]
    home = jnp.zeros((1, tokens), i32)
    for r in range(1, n):
        home = home + (own >= r * shard_rows).astype(i32)
    home_hot = home == iota((n, tokens), 0)
    ahead = jnp.dot(home_hot.astype(bf16), before, preferred_element_type=f32)
    rank = jnp.sum(jnp.where(home_hot, ahead, 0.0), axis=0, keepdims=True)
    arrive = home.astype(f32) * id_cap + rank
    arrive = jnp.transpose(jnp.broadcast_to(arrive, (8, tokens)))[:, 0:1].astype(i32)

    owner = pack[1:2, :]
    owner_hot = owner == iota((n, LANES), 0)
    before_slot = (iota((LANES, LANES), 0) < iota((LANES, LANES), 1)).astype(bf16)
    ahead = jnp.dot(owner_hot.astype(bf16), before_slot, preferred_element_type=f32)
    rank = jnp.sum(jnp.where(owner_hot, ahead, 0.0), axis=0, keepdims=True)
    slot_of = owner * cap + rank.astype(i32)
    selector = (slot_of == iota((n * cap, LANES), 0)).astype(f32)
    selector_ref[...] = selector[:, :slots].astype(bf16)

    for copy in id_copies:
        copy.wait()
    everyone = pack_recv[...]
    all_ids, all_routes = everyone[:, 0, :tokens], everyone[:, 1, :]
    relative = all_ids - s * shard_rows
    mine = (relative >= 0) & (relative < shard_rows)
    relative = jnp.where(mine, relative, 0)
    place = jnp.dot(mine.astype(bf16), upto, preferred_element_type=f32).astype(i32) - 1
    place = jnp.where(mine, place, -1)
    high, low = relative // LANES, relative % LANES
    found_high = jnp.zeros((n, id_cap), f32)
    found_low = jnp.zeros((n, id_cap), f32)
    row_n = iota((n, id_cap), 0)
    for t in range(n):
        hot = place[t : t + 1, :] == iota((id_cap, tokens), 0)
        hot_f = hot.astype(bf16)
        pick_dims = (((1,), (1,)), ((), ()))
        part = lax.dot_general(high.astype(bf16), hot_f, pick_dims, preferred_element_type=f32)
        found_high = jnp.where(row_n == t, part, found_high)
        part = lax.dot_general(low.astype(bf16), hot_f, pick_dims, preferred_element_type=f32)
        found_low = jnp.where(row_n == t, part, found_low)
        odd = jnp.sum(jnp.where(hot, relative[t : t + 1, :] % PAIR, 0).astype(f32), axis=1, keepdims=True)
        first = t * id_cap % (pick_ref.shape[1] // PAIR)
        rows = first + iota((id_cap, pick_ref.shape[1]), 0)
        chosen = rows * PAIR + odd.astype(i32) == iota((id_cap, pick_ref.shape[1]), 1)
        pick_ref[t * id_cap : (t + 1) * id_cap, :] = chosen.astype(f32).astype(bf16)
    local_ref[...] = (found_high * LANES + found_low).astype(i32)

    counts = jnp.sum((all_routes == s).astype(f32), axis=1, keepdims=True)
    spots = image_ref.shape[1]
    sender = iota((n, LANES), 1) // cap
    count_of = jnp.sum(jnp.where(sender == iota((n, LANES), 0), counts, 0.0), axis=0, keepdims=True)
    offset_of = jnp.sum(jnp.where(sender > iota((n, LANES), 0), counts, 0.0), axis=0, keepdims=True)
    within = iota((1, LANES), 1) % cap
    start = start_ref[0]
    position = jnp.where(
        within < count_of.astype(i32), start + offset_of.astype(i32) + within, -1
    )
    image = (position == iota((tokens, LANES), 0)).astype(f32)
    image_ref[...] = image[:, :spots].astype(bf16)
    total = jnp.sum(counts).astype(i32)
    row = iota((tokens, placed_ref.shape[1]), 0)
    is_text = (row < start) | (row >= start + total)
    hot = (arrive == iota((tokens, placed_ref.shape[1]), 1)) & is_text
    placed_ref[...] = hot.astype(f32).astype(bf16)

    for copy in x_copies:
        copy.wait()
    x_ref[...] = x_recv[...]


def exchange(token_ids, routes, splice_start, vision, gain, table_rows, depth):
    n, voc = lax.axis_size("seq"), lax.axis_size("vocab")
    tokens, slots = token_ids.shape[0], routes.shape[0]
    block = n * slots // (2 * voc)
    blocks = slots // block
    id_cap, cap = 2 * tokens // n, 2 * slots // n
    i32, bf16 = jnp.int32, jnp.bfloat16
    vmem = pl.BlockSpec(memory_space=pltpu.VMEM)
    smem = pl.BlockSpec(memory_space=pltpu.SMEM)
    dma = pltpu.SemaphoreType.DMA
    shape = jax.ShapeDtypeStruct
    held = PAIR * min(n * id_cap, 128)

    def body(*refs):
        exchange_kernel(table_rows, *refs)

    return pl.pallas_call(
        body,
        out_shape=(
            shape((n, id_cap), i32),
            shape((n * id_cap, held), bf16),
            shape((n * cap, slots), bf16),
            shape((tokens, n * cap), bf16),
            shape((tokens, n * id_cap), bf16),
            shape((2, voc, block, depth), bf16),
        ),
        in_specs=[vmem, vmem, smem, vmem, vmem],
        out_specs=(vmem,) * 6,
        scratch_shapes=[
            pltpu.VMEM((8, LANES), i32),
            pltpu.VMEM((n, 8, LANES), i32),
            pltpu.VMEM((n, blocks, block, depth), bf16),
            pltpu.VMEM((2, voc, block, depth), bf16),
            dma((2, n)),
            dma((2, n)),
        ],
        compiler_params=pltpu.CompilerParams(
            collective_id=1, has_side_effects=True, vmem_limit_bytes=16 * 1024 * 1024
        ),
        name="exchange",
    )(token_ids[None, :], routes.reshape(1, slots), splice_start, vision, gain[None, :])


def gather_kernel(ids_ref, pick_ref, table_ref, out_ref, held, sems):
    groups, cap = ids_ref.shape
    span = pick_ref.shape[1]
    per = span // (PAIR * cap)

    def issue(g, carry):
        for k in range(cap):
            row = pl.multiple_of(ids_ref[g, k] // PAIR * PAIR, PAIR)
            spot = pl.multiple_of((g * cap + k) * PAIR, PAIR)
            pltpu.make_async_copy(
                table_ref.at[pl.ds(row, PAIR), :], held.at[pl.ds(spot, PAIR), :], sems.at[g // per]
            ).start()
        return carry

    lax.fori_loop(0, groups, issue, 0)

    for g in range(groups // per):
        block = held.at[g * span : (g + 1) * span, :]
        pltpu.make_async_copy(block, block, sems.at[g]).wait()
        rows = slice(g * per * cap, (g + 1) * per * cap)
        for k in range(0, held.shape[1], 256):
            found = jnp.dot(
                pick_ref[rows, :], block[:, k : k + 256], preferred_element_type=jnp.float32
            )
            out_ref[rows, k : k + 256] = found.astype(out_ref.dtype)


def gather_rows(local_ids, pick, table):
    groups, cap = local_ids.shape
    width = table.shape[1]
    found = pl.pallas_call(
        gather_kernel,
        out_shape=jax.ShapeDtypeStruct((groups * cap, width), table.dtype),
        in_specs=[
            pl.BlockSpec(memory_space=pltpu.SMEM),
            pl.BlockSpec(memory_space=pltpu.VMEM),
            pl.BlockSpec(memory_space=pl.ANY),
        ],
        out_specs=pl.BlockSpec(memory_space=pltpu.VMEM),
        scratch_shapes=[
            pltpu.VMEM((groups * cap * PAIR, width), table.dtype),
            pltpu.SemaphoreType.DMA((groups * cap * PAIR // pick.shape[1],)),
        ],
        name="gather_rows",
    )(local_ids, pick, table)
    return found.reshape(groups, cap, width)


def mega_kernel(
    x_ref, w1_hbm, w2_hbm, text_ref, selector_ref, image_ref, placed_ref, out_ref,
    w1, w2, half_send, half_recv, half_own, plane_send, plane_recv, cross_recv,
    h_own, h_recv, pair_send, pair_recv, pair_own, part_send, part_recv,
    row_send, row_recv, text_recv, total,
    w_sem, half_sems, plane_sems, cross_sems, h_sems,
    pair_sems, part_sems, row_sems, text_sems,
):
    n, voc = lax.axis_size("seq"), lax.axis_size("vocab")
    s, v = lax.axis_index("seq"), lax.axis_index("vocab")
    chips = n // 2
    z, c = s // 2, s % 2
    split = n // voc
    f32, bf16 = jnp.float32, jnp.bfloat16
    block = x_ref.shape[2]
    slots = voc * block // chips
    blocks = slots // block

    load1 = pltpu.make_async_copy(w1_hbm, w1, w_sem.at[0])
    load2 = pltpu.make_async_copy(w2_hbm, w2, w_sem.at[1])
    load1.start()
    load2.start()

    barrier = pltpu.get_barrier_semaphore()
    for d in range(1, n):
        pl.semaphore_signal(barrier, inc=1, **at(lax.rem(s + d, n), v))
    for e in range(1, voc):
        pl.semaphore_signal(barrier, inc=1, **at(s, lax.rem(v + e, voc)))

    pl.semaphore_wait(barrier, n - 1 + voc - 1)

    def to_peer(source, target, sems, d, seq, vocab=None):
        copy = pltpu.make_async_remote_copy(
            src_ref=source,
            dst_ref=target,
            send_sem=sems.at[0, d],
            recv_sem=sems.at[1, d],
            **at(seq, v if vocab is None else vocab),
        )
        copy.start()
        return copy

    texts = []

    def send_text(ds):
        for d in ds:
            peer = lax.rem(s + d, n)
            texts.append(to_peer(text_ref.at[peer], text_recv.at[s], text_sems, d, peer))

    send_text(TEXT_A(n))
    stay = pltpu.make_async_copy(text_ref.at[s], text_recv.at[s], w_sem.at[2])
    stay.start()

    def columns(width):
        return 256 if width % 256 == 0 else width

    def chip_sums(lhs_ref, weight, to_sib, from_sib, own, sems_pair):
        width = weight.shape[1]
        step = columns(width)
        for core, keep in ((1 - c, False), (c, True)):
            lhs = lhs_ref[core].reshape(-1, weight.shape[0])
            for k in range(0, width, step):
                part = jnp.dot(lhs, weight[:, k : k + step], preferred_element_type=f32)
                if keep:
                    own[:, k : k + step] = part
                else:
                    to_sib[:, k : k + step] = part.astype(bf16)
            if not keep:
                swap = to_peer(to_sib, from_sib, sems_pair, 0, s + 1 - 2 * c)
        swap.wait()

    load1.wait()
    chip_sums(x_ref, w1, half_send, half_recv, half_own, half_sems)
    copies = []
    for e in range(1, voc):
        peer = lax.rem(v + e, voc)
        span = pl.ds(pl.multiple_of(peer * block, block), block)
        plane_send[e] = (half_own[span, :] + half_recv[span, :].astype(f32)).astype(bf16)
        copies.append(to_peer(plane_send.at[e], plane_recv.at[v], plane_sems, e, s, peer))
    send_text(TEXT_B(n))
    span = pl.ds(pl.multiple_of(v * block, block), block)
    plane_recv[v] = (half_own[span, :] + half_recv[span, :].astype(f32)).astype(bf16)
    for copy in copies:
        copy.wait()

    inner = h_own.shape[2]

    def hidden_part(seq):
        side = pl.multiple_of(seq % split * inner, inner) if split > 1 else 0
        return plane_recv.at[seq // split, :, pl.ds(side, inner)]

    copies = []
    for d in range(1, n):
        peer = lax.rem(s + d, n)
        copies.append(to_peer(hidden_part(peer), cross_recv.at[s], cross_sems, d, peer))
    cross_recv[s] = hidden_part(s)[...]
    send_text(TEXT_C(n))
    for copy in copies:
        copy.wait()
    for core in range(2):
        pre = cross_recv[core].astype(f32)
        for k in range(1, chips):
            pre = pre + cross_recv[2 * k + core].astype(f32)
        h_own[core] = (0.5 * pre * (1.0 + lax.erf(pre * math.sqrt(0.5)))).astype(bf16)

    def h_place(vocab):
        if blocks == 1:
            return h_recv.at[:, vocab, 0]
        return h_recv.at[vocab % 2, vocab // 2]

    copies = []
    for e in range(1, voc):
        peer = lax.rem(v + e, voc)
        copies.append(to_peer(h_own, h_place(v), h_sems, e, s, peer))
    h_place(v)[...] = h_own[...]
    load2.wait()
    for copy in copies:
        copy.wait()

    width = w2.shape[1]
    chip_sums(h_recv, w2, pair_send, pair_recv, pair_own, pair_sems)
    sent = []
    for d in range(1, chips):
        other = lax.rem(z + d, chips)
        span = pl.ds(pl.multiple_of(other * slots, slots), slots)
        part_send[d] = (pair_own[span, :] + pair_recv[span, :].astype(f32)).astype(bf16)
        sent.append(to_peer(part_send.at[d], part_recv.at[d], part_sems, d, other * 2 + c))
    send_text(TEXT_D(n))
    span = pl.ds(pl.multiple_of(z * slots, slots), slots)
    value = pair_own[span, :] + pair_recv[span, :].astype(f32)
    for copy in sent:
        copy.wait()
    for d in range(1, chips):
        value = value + part_recv[d].astype(f32)
    merged = value.astype(bf16)

    cap = row_send.shape[1]
    outgoing = jnp.dot(selector_ref[...], merged, preferred_element_type=f32).astype(bf16)
    for t in range(n):
        row_send[t] = outgoing[t * cap : (t + 1) * cap]
    copies = []
    for d in range(1, n):
        peer = lax.rem(s + d, n)
        copies.append(to_peer(row_send.at[peer], row_recv.at[s], row_sems, d, peer))
    row_recv[s] = row_send[s]
    for copy in texts:
        copy.wait()
    stay.wait()
    step = columns(width)
    found = text_recv[...].reshape(-1, width)
    for k in range(0, width, step):
        total[:, k : k + step] = jnp.dot(
            placed_ref[...], found[:, k : k + step], preferred_element_type=f32
        )
    for copy in copies:
        copy.wait()
    for k in range(0, width, step):
        value = total[:, k : k + step]
        block_rows = row_recv[:, :, k : k + step].astype(f32).reshape(n * cap, step).astype(bf16)
        value = value + jnp.dot(image_ref[...], block_rows, preferred_element_type=f32)
        out_ref[:, k : k + step] = value.astype(bf16)


def TEXT_A(n):
    return range(1, 2)


def TEXT_B(n):
    return range(2, n // 2)


def TEXT_C(n):
    return range(n // 2, 3 * n // 4)


def TEXT_D(n):
    return range(3 * n // 4, n)


def mega(x, w1, w2, text, selector, image_pick, text_pick):
    n, voc = lax.axis_size("seq"), lax.axis_size("vocab")
    block = x.shape[2]
    slots = 2 * voc * block // n
    rows = n // 2 * slots
    blocks = slots // block
    depth, mid = w1.shape
    inner, width = w2.shape
    cap = selector.shape[0] // n
    bf16, f32 = jnp.bfloat16, jnp.float32
    vmem = pl.BlockSpec(memory_space=pltpu.VMEM)
    hbm = pl.BlockSpec(memory_space=pl.ANY)
    dma = pltpu.SemaphoreType.DMA
    return pl.pallas_call(
        mega_kernel,
        out_shape=jax.ShapeDtypeStruct((image_pick.shape[0], width), bf16),
        in_specs=[vmem, hbm, hbm, hbm, vmem, vmem, vmem],
        out_specs=vmem,
        scratch_shapes=[
            pltpu.VMEM(w1.shape, bf16),
            pltpu.VMEM(w2.shape, bf16),
            pltpu.VMEM((voc * block, mid), bf16),
            pltpu.VMEM((voc * block, mid), bf16),
            pltpu.VMEM((voc * block, mid), f32),
            pltpu.VMEM((voc, block, mid), bf16),
            pltpu.VMEM((voc, block, mid), bf16),
            pltpu.VMEM((n, block, inner), bf16),
            pltpu.VMEM((2, block, inner), bf16),
            pltpu.VMEM((2, n // 2, blocks, block, inner), bf16),
            pltpu.VMEM((rows, width), bf16),
            pltpu.VMEM((rows, width), bf16),
            pltpu.VMEM((rows, width), f32),
            pltpu.VMEM((n // 2, slots, width), bf16),
            pltpu.VMEM((n // 2, slots, width), bf16),
            pltpu.VMEM((n, cap, width), bf16),
            pltpu.VMEM((n, cap, width), bf16),
            pltpu.VMEM(text.shape, bf16),
            pltpu.VMEM((image_pick.shape[0], width), f32),
            dma((3,)),
            dma((2, 1)),
            dma((2, voc)),
            dma((2, n)),
            dma((2, voc)),
            dma((2, 1)),
            dma((2, n // 2)),
            dma((2, n)),
            dma((2, n)),
        ],
        compiler_params=pltpu.CompilerParams(
            collective_id=0, has_side_effects=True, vmem_limit_bytes=56 * 1024 * 1024
        ),
        name="merger",
    )(x, w1, w2, text, selector, image_pick, text_pick)


def on_device(token_ids, routes, splice_start, vision, ln_gain, table, w_fc1, w_fc2):
    local_ids, pick, selector, image_pick, text_pick, x = exchange(
        token_ids, routes, splice_start, vision, ln_gain, table.shape[0], w_fc1.shape[0]
    )
    text = gather_rows(local_ids, pick, table)
    return mega(x, w_fc1, w_fc2, text, selector, image_pick, text_pick)


def solution(mesh):
    in_specs = (
        P("seq"),
        P("seq", None),
        P("seq"),
        P("seq", None),
        P(),
        P("seq", "vocab"),
        P("seq", "vocab"),
        P("seq", "vocab"),
    )
    out_specs = P("seq", "vocab")
    return jax.shard_map(
        on_device, mesh=mesh, in_specs=in_specs, out_specs=out_specs, check_vma=False
    )
```

```python
import math

import jax
import jax.numpy as jnp
from jax import lax
from jax.experimental import pallas as pl
from jax.experimental.pallas import tpu as pltpu
from jax.sharding import PartitionSpec as P


PAIR = 2
LANES = 128


def at(seq, vocab):
    return dict(device_id=(seq, vocab), device_id_type=pl.DeviceIdType.MESH)


def iota(shape, dim):
    return lax.broadcasted_iota(jnp.int32, shape, dim)


def in_hbm(array):
    return pltpu.with_memory_space_constraint(array, pltpu.HBM)


def x_slot(ref, seq, blocks):
    if blocks == 1:
        return ref.at[pl.ds(seq % 2, 1), seq // 2]
    return ref.at[:, seq]


def exchange_kernel(
    shard_rows, ids_hbm, routes_hbm, start_ref, vision_hbm, gain_hbm,
    local_ref, pick_ref, selector_ref, image_ref, placed_ref, x_ref,
    ids_ref, routes_ref, vision_ref, gain_ref,
    pack, pack_recv, x_send, x_recv, load_sems, id_sems, x_sems,
):
    n = lax.axis_size("seq")
    s, v = lax.axis_index("seq"), lax.axis_index("vocab")
    f32, bf16, i32 = jnp.float32, jnp.bfloat16, jnp.int32
    tokens, slots = ids_ref.shape[1], routes_ref.shape[1]
    id_cap = local_ref.shape[1]
    cap = selector_ref.shape[0] // n
    blocks, block, depth = x_send.shape[1:]

    loads = [
        pltpu.make_async_copy(source, target, load_sems.at[k])
        for k, (source, target) in enumerate((
            (vision_hbm, vision_ref), (gain_hbm, gain_ref), (ids_hbm, ids_ref), (routes_hbm, routes_ref)
        ))
    ]
    for load in loads:
        load.start()
    barrier = pltpu.get_barrier_semaphore()
    for d in range(1, n):
        pl.semaphore_signal(barrier, inc=1, **at(lax.rem(s + d, n), v))
    for load in loads:
        load.wait()

    pack[...] = jnp.full(pack.shape, -1, i32)
    pack[0:1, :tokens] = ids_ref[...]
    pack[1:2, :slots] = routes_ref[...]
    pack_recv[s] = pack[...]

    group = gain_ref.shape[0]
    gain = gain_ref[...][None, :]
    for g in range(vision_ref.shape[1] // group):
        values = vision_ref[:, g * group : (g + 1) * group].astype(f32)
        center = values - jnp.mean(values, axis=-1, keepdims=True)
        spread = jnp.mean(center * center, axis=-1, keepdims=True)
        normed = (center / jnp.sqrt(spread + 1e-06) * gain).astype(bf16)
        for k in range(group // depth):
            part = normed[:, k * depth : (k + 1) * depth]
            for i in range(blocks):
                x_send[g * (group // depth) + k, i] = part[i * block : (i + 1) * block]

    pl.semaphore_wait(barrier, n - 1)

    def to_peer(source, target, sems, d, seq):
        copy = pltpu.make_async_remote_copy(
            src_ref=source,
            dst_ref=target,
            send_sem=sems.at[0, d],
            recv_sem=sems.at[1, d],
            **at(seq, v),
        )
        copy.start()
        return copy

    id_copies, x_copies = [], []
    for d in range(1, n):
        peer = lax.rem(s + d, n)
        id_copies.append(to_peer(pack, pack_recv.at[s], id_sems, d, peer))
    for d in range(1, n):
        peer = lax.rem(s + d, n)
        x_copies.append(
            to_peer(x_send.at[peer], x_slot(x_recv, s, blocks), x_sems, d, peer)
        )
    x_slot(x_recv, s, blocks)[...] = x_send[s]

    lane_t = iota((tokens, tokens), 1)
    upto = (iota((tokens, tokens), 0) <= lane_t).astype(bf16)
    before = (iota((tokens, tokens), 0) < lane_t).astype(bf16)

    own = ids_ref[...]
    home = jnp.zeros((1, tokens), i32)
    for r in range(1, n):
        home = home + (own >= r * shard_rows).astype(i32)
    home_hot = home == iota((n, tokens), 0)
    ahead = jnp.dot(home_hot.astype(bf16), before, preferred_element_type=f32)
    rank = jnp.sum(jnp.where(home_hot, ahead, 0.0), axis=0, keepdims=True)
    arrive = home.astype(f32) * id_cap + rank
    arrive = jnp.transpose(jnp.broadcast_to(arrive, (8, tokens)))[:, 0:1].astype(i32)

    owner = pack[1:2, :]
    owner_hot = owner == iota((n, LANES), 0)
    before_slot = (iota((LANES, LANES), 0) < iota((LANES, LANES), 1)).astype(bf16)
    ahead = jnp.dot(owner_hot.astype(bf16), before_slot, preferred_element_type=f32)
    rank = jnp.sum(jnp.where(owner_hot, ahead, 0.0), axis=0, keepdims=True)
    slot_of = owner * cap + rank.astype(i32)
    selector = (slot_of == iota((n * cap, LANES), 0)).astype(f32)
    selector_ref[...] = selector[:, :slots].astype(bf16)

    for copy in id_copies:
        copy.wait()
    everyone = pack_recv[...]
    all_ids, all_routes = everyone[:, 0, :tokens], everyone[:, 1, :]
    relative = all_ids - s * shard_rows
    mine = (relative >= 0) & (relative < shard_rows)
    relative = jnp.where(mine, relative, 0)
    place = jnp.dot(mine.astype(bf16), upto, preferred_element_type=f32).astype(i32) - 1
    place = jnp.where(mine, place, -1)
    high, low = relative // LANES, relative % LANES
    found_high = jnp.zeros((n, id_cap), f32)
    found_low = jnp.zeros((n, id_cap), f32)
    row_n = iota((n, id_cap), 0)
    for t in range(n):
        hot = place[t : t + 1, :] == iota((id_cap, tokens), 0)
        hot_f = hot.astype(bf16)
        pick_dims = (((1,), (1,)), ((), ()))
        part = lax.dot_general(high.astype(bf16), hot_f, pick_dims, preferred_element_type=f32)
        found_high = jnp.where(row_n == t, part, found_high)
        part = lax.dot_general(low.astype(bf16), hot_f, pick_dims, preferred_element_type=f32)
        found_low = jnp.where(row_n == t, part, found_low)
        odd = jnp.sum(jnp.where(hot, relative[t : t + 1, :] % PAIR, 0).astype(f32), axis=1, keepdims=True)
        first = t * id_cap % (pick_ref.shape[1] // PAIR)
        rows = first + iota((id_cap, pick_ref.shape[1]), 0)
        chosen = rows * PAIR + odd.astype(i32) == iota((id_cap, pick_ref.shape[1]), 1)
        pick_ref[t * id_cap : (t + 1) * id_cap, :] = chosen.astype(f32).astype(bf16)
    local_ref[...] = (found_high * LANES + found_low).astype(i32)

    counts = jnp.sum((all_routes == s).astype(f32), axis=1, keepdims=True)
    spots = image_ref.shape[1]
    sender = iota((n, LANES), 1) // cap
    count_of = jnp.sum(jnp.where(sender == iota((n, LANES), 0), counts, 0.0), axis=0, keepdims=True)
    offset_of = jnp.sum(jnp.where(sender > iota((n, LANES), 0), counts, 0.0), axis=0, keepdims=True)
    within = iota((1, LANES), 1) % cap
    start = start_ref[0]
    position = jnp.where(
        within < count_of.astype(i32), start + offset_of.astype(i32) + within, -1
    )
    image = (position == iota((tokens, LANES), 0)).astype(f32)
    image_ref[...] = image[:, :spots].astype(bf16)
    total = jnp.sum(counts).astype(i32)
    row = iota((tokens, placed_ref.shape[1]), 0)
    is_text = (row < start) | (row >= start + total)
    hot = (arrive == iota((tokens, placed_ref.shape[1]), 1)) & is_text
    placed_ref[...] = hot.astype(f32).astype(bf16)

    for copy in x_copies:
        copy.wait()
    x_ref[...] = x_recv[...]


def exchange(token_ids, routes, splice_start, vision, gain, table_rows, depth):
    n, voc = lax.axis_size("seq"), lax.axis_size("vocab")
    tokens, slots = token_ids.shape[0], routes.shape[0]
    block = n * slots // (2 * voc)
    blocks = slots // block
    id_cap, cap = 2 * tokens // n, 2 * slots // n
    i32, bf16 = jnp.int32, jnp.bfloat16
    vmem = pl.BlockSpec(memory_space=pltpu.VMEM)
    smem = pl.BlockSpec(memory_space=pltpu.SMEM)
    hbm = pl.BlockSpec(memory_space=pltpu.HBM)
    dma = pltpu.SemaphoreType.DMA
    shape = jax.ShapeDtypeStruct
    held = PAIR * min(n * id_cap, 128)

    def body(*refs):
        exchange_kernel(table_rows, *refs)

    return pl.pallas_call(
        body,
        out_shape=(
            shape((n, id_cap), i32),
            shape((n * id_cap, held), bf16),
            shape((n * cap, slots), bf16),
            shape((tokens, n * cap), bf16),
            shape((tokens, n * id_cap), bf16),
            shape((2, voc, block, depth), bf16),
        ),
        in_specs=[hbm, hbm, smem, hbm, hbm],
        out_specs=(vmem,) * 6,
        scratch_shapes=[
            pltpu.VMEM((1, tokens), i32),
            pltpu.VMEM((1, slots), i32),
            pltpu.VMEM(vision.shape, vision.dtype),
            pltpu.VMEM(gain.shape, gain.dtype),
            pltpu.VMEM((8, LANES), i32),
            pltpu.VMEM((n, 8, LANES), i32),
            pltpu.VMEM((n, blocks, block, depth), bf16),
            pltpu.VMEM((2, voc, block, depth), bf16),
            dma((4,)),
            dma((2, n)),
            dma((2, n)),
        ],
        compiler_params=pltpu.CompilerParams(
            collective_id=1, has_side_effects=True, vmem_limit_bytes=16 * 1024 * 1024
        ),
        name="exchange",
    )(
        in_hbm(token_ids[None, :]),
        in_hbm(routes.reshape(1, slots)),
        splice_start,
        in_hbm(vision),
        in_hbm(gain),
    )


def columns(width):
    return 256 if width % 256 == 0 else width


def gather_kernel(
    ids_ref, pick_ref, x_ref, table_ref, w1_hbm, out_ref, sib_ref, own_ref, w1, held, sems, w_sem
):
    groups, cap = ids_ref.shape
    span = pick_ref.shape[1]
    per = span // (PAIR * cap)
    core = lax.axis_index("seq") % 2
    load = pltpu.make_async_copy(w1_hbm, w1, w_sem)
    load.start()

    def issue(g, carry):
        for k in range(cap):
            row = pl.multiple_of(ids_ref[g, k] // PAIR * PAIR, PAIR)
            spot = pl.multiple_of((g * cap + k) * PAIR, PAIR)
            pltpu.make_async_copy(
                table_ref.at[pl.ds(row, PAIR), :], held.at[pl.ds(spot, PAIR), :], sems.at[g // per]
            ).start()
        return carry

    lax.fori_loop(0, groups, issue, 0)

    load.wait()
    mid = w1.shape[1]
    step = columns(mid)
    theirs = x_ref[1 - core].reshape(-1, w1.shape[0])
    ours = x_ref[core].reshape(-1, w1.shape[0])
    for k in range(0, mid, step):
        weight = w1[:, k : k + step]
        sib_ref[:, k : k + step] = jnp.dot(
            theirs, weight, preferred_element_type=jnp.float32
        ).astype(sib_ref.dtype)
        own_ref[:, k : k + step] = jnp.dot(ours, weight, preferred_element_type=jnp.float32)

    for g in range(groups // per):
        block = held.at[g * span : (g + 1) * span, :]
        pltpu.make_async_copy(block, block, sems.at[g]).wait()
        rows = slice(g * per * cap, (g + 1) * per * cap)
        for k in range(0, held.shape[1], 256):
            found = jnp.dot(
                pick_ref[rows, :], block[:, k : k + 256], preferred_element_type=jnp.float32
            )
            out_ref[rows, k : k + 256] = found.astype(out_ref.dtype)


def gather_rows(local_ids, pick, x, table, w1):
    groups, cap = local_ids.shape
    width = table.shape[1]
    rows, mid = x.shape[1] * x.shape[2], w1.shape[1]
    vmem = pl.BlockSpec(memory_space=pltpu.VMEM)
    hbm = pl.BlockSpec(memory_space=pltpu.HBM)
    shape = jax.ShapeDtypeStruct
    found, theirs, ours = pl.pallas_call(
        gather_kernel,
        out_shape=(
            shape((groups * cap, width), table.dtype),
            shape((rows, mid), jnp.bfloat16),
            shape((rows, mid), jnp.float32),
        ),
        in_specs=[pl.BlockSpec(memory_space=pltpu.SMEM), vmem, vmem, hbm, hbm],
        out_specs=(vmem,) * 3,
        scratch_shapes=[
            pltpu.VMEM(w1.shape, w1.dtype),
            pltpu.VMEM((groups * cap * PAIR, width), table.dtype),
            pltpu.SemaphoreType.DMA((groups * cap * PAIR // pick.shape[1],)),
            pltpu.SemaphoreType.DMA,
        ],
        compiler_params=pltpu.CompilerParams(vmem_limit_bytes=16 * 1024 * 1024),
        name="gather_rows",
    )(local_ids, pick, x, table, in_hbm(w1))
    return found.reshape(groups, cap, width), theirs, ours


def mega_kernel(
    half_send, half_own, w2_hbm, text_ref, selector_ref, image_ref, placed_ref, out_ref,
    w2, half_recv, plane_send, plane_recv, cross_recv,
    h_own, h_recv, pair_send, pair_recv, pair_own, part_send, part_recv,
    row_send, row_recv, text_recv, total,
    w_sem, half_sems, plane_sems, cross_sems, h_sems,
    pair_sems, part_sems, row_sems, text_sems,
):
    n, voc = lax.axis_size("seq"), lax.axis_size("vocab")
    s, v = lax.axis_index("seq"), lax.axis_index("vocab")
    chips = n // 2
    z, c = s // 2, s % 2
    split = n // voc
    f32, bf16 = jnp.float32, jnp.bfloat16
    block = plane_recv.shape[1]
    slots = voc * block // chips
    blocks = slots // block

    load2 = pltpu.make_async_copy(w2_hbm, w2, w_sem.at[0])
    load2.start()

    barrier = pltpu.get_barrier_semaphore()
    for d in range(1, n):
        pl.semaphore_signal(barrier, inc=1, **at(lax.rem(s + d, n), v))
    for e in range(1, voc):
        pl.semaphore_signal(barrier, inc=1, **at(s, lax.rem(v + e, voc)))

    pl.semaphore_wait(barrier, n - 1 + voc - 1)

    def to_peer(source, target, sems, d, seq, vocab=None):
        copy = pltpu.make_async_remote_copy(
            src_ref=source,
            dst_ref=target,
            send_sem=sems.at[0, d],
            recv_sem=sems.at[1, d],
            **at(seq, v if vocab is None else vocab),
        )
        copy.start()
        return copy

    swap = to_peer(half_send, half_recv, half_sems, 0, s + 1 - 2 * c)
    texts = []

    def send_text(ds):
        for d in ds:
            peer = lax.rem(s + d, n)
            texts.append(to_peer(text_ref.at[peer], text_recv.at[s], text_sems, d, peer))

    send_text(text_turns(n, 0))
    swap.wait()

    def chip_sums(lhs_ref, weight, to_sib, from_sib, own, sems_pair):
        width = weight.shape[1]
        step = columns(width)
        for core, keep in ((1 - c, False), (c, True)):
            lhs = lhs_ref[core].reshape(-1, weight.shape[0])
            for k in range(0, width, step):
                part = jnp.dot(lhs, weight[:, k : k + step], preferred_element_type=f32)
                if keep:
                    own[:, k : k + step] = part
                else:
                    to_sib[:, k : k + step] = part.astype(bf16)
            if not keep:
                swap = to_peer(to_sib, from_sib, sems_pair, 0, s + 1 - 2 * c)
        swap.wait()

    copies = []
    for e in range(1, voc):
        peer = lax.rem(v + e, voc)
        span = pl.ds(pl.multiple_of(peer * block, block), block)
        plane_send[e] = (half_own[span, :] + half_recv[span, :].astype(f32)).astype(bf16)
        copies.append(to_peer(plane_send.at[e], plane_recv.at[v], plane_sems, e, s, peer))
    text_recv[s] = text_ref[s]
    send_text(text_turns(n, 1))
    span = pl.ds(pl.multiple_of(v * block, block), block)
    plane_recv[v] = (half_own[span, :] + half_recv[span, :].astype(f32)).astype(bf16)
    for copy in copies:
        copy.wait()

    inner = h_own.shape[2]

    def hidden_part(seq):
        side = pl.multiple_of(seq % split * inner, inner) if split > 1 else 0
        return plane_recv.at[seq // split, :, pl.ds(side, inner)]

    copies = []
    for d in range(1, n):
        peer = lax.rem(s + d, n)
        copies.append(to_peer(hidden_part(peer), cross_recv.at[s], cross_sems, d, peer))
    cross_recv[s] = hidden_part(s)[...]
    send_text(text_turns(n, 2))
    for copy in copies:
        copy.wait()
    for core in range(2):
        pre = cross_recv[core].astype(f32)
        for k in range(1, chips):
            pre = pre + cross_recv[2 * k + core].astype(f32)
        h_own[core] = (0.5 * pre * (1.0 + lax.erf(pre * math.sqrt(0.5)))).astype(bf16)

    def h_place(vocab):
        if blocks == 1:
            return h_recv.at[:, vocab, 0]
        return h_recv.at[vocab % 2, vocab // 2]

    copies = []
    for e in range(1, voc):
        peer = lax.rem(v + e, voc)
        copies.append(to_peer(h_own, h_place(v), h_sems, e, s, peer))
    send_text(text_turns(n, 3))
    h_place(v)[...] = h_own[...]
    load2.wait()
    for copy in copies:
        copy.wait()

    width = w2.shape[1]
    chip_sums(h_recv, w2, pair_send, pair_recv, pair_own, pair_sems)
    sent = []
    for d in range(1, chips):
        other = lax.rem(z + d, chips)
        span = pl.ds(pl.multiple_of(other * slots, slots), slots)
        part_send[d] = (pair_own[span, :] + pair_recv[span, :].astype(f32)).astype(bf16)
        sent.append(to_peer(part_send.at[d], part_recv.at[d], part_sems, d, other * 2 + c))
    send_text(text_turns(n, 4))
    span = pl.ds(pl.multiple_of(z * slots, slots), slots)
    value = pair_own[span, :] + pair_recv[span, :].astype(f32)
    for copy in sent:
        copy.wait()
    for d in range(1, chips):
        value = value + part_recv[d].astype(f32)
    merged = value.astype(bf16)

    cap = row_send.shape[1]
    outgoing = jnp.dot(selector_ref[...], merged, preferred_element_type=f32).astype(bf16)
    for t in range(n):
        row_send[t] = outgoing[t * cap : (t + 1) * cap]
    copies = []
    for d in range(1, n):
        peer = lax.rem(s + d, n)
        copies.append(to_peer(row_send.at[peer], row_recv.at[s], row_sems, d, peer))
    row_recv[s] = row_send[s]
    for copy in texts:
        copy.wait()
    step = columns(width)
    found = text_recv[...].reshape(-1, width)
    for k in range(0, width, step):
        total[:, k : k + step] = jnp.dot(
            placed_ref[...], found[:, k : k + step], preferred_element_type=f32
        )
    for copy in copies:
        copy.wait()
    for k in range(0, width, step):
        value = total[:, k : k + step]
        block_rows = row_recv[:, :, k : k + step].astype(f32).reshape(n * cap, step).astype(bf16)
        value = value + jnp.dot(image_ref[...], block_rows, preferred_element_type=f32)
        out_ref[:, k : k + step] = value.astype(bf16)


CUTS = (1, 3, 5, 8, 8)


def text_turns(n, turn):
    order = sorted(range(1, n), key=lambda d: -min(d, n - d))
    edges = [0] + [cut * n // 8 for cut in CUTS]
    return order[edges[turn] : edges[turn + 1]]


def mega(theirs, ours, w2, text, selector, image_pick, text_pick):
    n, voc = lax.axis_size("seq"), lax.axis_size("vocab")
    rows, mid = theirs.shape
    block = rows // voc
    slots = 2 * rows // n
    blocks = slots // block
    inner, width = w2.shape
    cap = selector.shape[0] // n
    bf16, f32 = jnp.bfloat16, jnp.float32
    vmem = pl.BlockSpec(memory_space=pltpu.VMEM)
    hbm = pl.BlockSpec(memory_space=pltpu.HBM)
    dma = pltpu.SemaphoreType.DMA
    return pl.pallas_call(
        mega_kernel,
        out_shape=jax.ShapeDtypeStruct((image_pick.shape[0], width), bf16),
        in_specs=[vmem, vmem, hbm, vmem, vmem, vmem, vmem],
        out_specs=vmem,
        scratch_shapes=[
            pltpu.VMEM(w2.shape, bf16),
            pltpu.VMEM(theirs.shape, bf16),
            pltpu.VMEM((voc, block, mid), bf16),
            pltpu.VMEM((voc, block, mid), bf16),
            pltpu.VMEM((n, block, inner), bf16),
            pltpu.VMEM((2, block, inner), bf16),
            pltpu.VMEM((2, n // 2, blocks, block, inner), bf16),
            pltpu.VMEM((rows, width), bf16),
            pltpu.VMEM((rows, width), bf16),
            pltpu.VMEM((rows, width), f32),
            pltpu.VMEM((n // 2, slots, width), bf16),
            pltpu.VMEM((n // 2, slots, width), bf16),
            pltpu.VMEM((n, cap, width), bf16),
            pltpu.VMEM((n, cap, width), bf16),
            pltpu.VMEM(text.shape, bf16),
            pltpu.VMEM((image_pick.shape[0], width), f32),
            dma((1,)),
            dma((2, 1)),
            dma((2, voc)),
            dma((2, n)),
            dma((2, voc)),
            dma((2, 1)),
            dma((2, n // 2)),
            dma((2, n)),
            dma((2, n)),
        ],
        compiler_params=pltpu.CompilerParams(
            collective_id=0, has_side_effects=True, vmem_limit_bytes=24 * 1024 * 1024
        ),
        name="merger",
    )(theirs, ours, in_hbm(w2), text, selector, image_pick, text_pick)


def on_device(token_ids, routes, splice_start, vision, ln_gain, table, w_fc1, w_fc2):
    local_ids, pick, selector, image_pick, text_pick, x = exchange(
        token_ids, routes, splice_start, vision, ln_gain, table.shape[0], w_fc1.shape[0]
    )
    text, theirs, ours = gather_rows(local_ids, pick, x, table, w_fc1)
    return mega(theirs, ours, w_fc2, text, selector, image_pick, text_pick)


def solution(mesh):
    in_specs = (
        P("seq"),
        P("seq", None),
        P("seq"),
        P("seq", None),
        P(),
        P("seq", "vocab"),
        P("seq", "vocab"),
        P("seq", "vocab"),
    )
    out_specs = P("seq", "vocab")
    return jax.shard_map(
        on_device, mesh=mesh, in_specs=in_specs, out_specs=out_specs, check_vma=False
    )
```

```python
import math

import jax
import jax.numpy as jnp
from jax import lax
from jax.experimental import pallas as pl
from jax.experimental.pallas import tpu as pltpu
from jax.sharding import PartitionSpec as P


PAIR = 2
LANES = 128


def at(seq, vocab):
    return dict(device_id=(seq, vocab), device_id_type=pl.DeviceIdType.MESH)


def iota(shape, dim):
    return lax.broadcasted_iota(jnp.int32, shape, dim)


def in_hbm(array):
    return pltpu.with_memory_space_constraint(array, pltpu.HBM)


def x_slot(ref, seq, blocks):
    if blocks == 1:
        return ref.at[pl.ds(seq % 2, 1), seq // 2]
    return ref.at[:, seq]


def exchange_kernel(
    shard_rows, ids_hbm, routes_hbm, start_ref, vision_hbm, gain_hbm,
    local_ref, pick_ref, selector_ref, image_ref, placed_ref, x_ref,
    ids_ref, routes_ref, vision_ref, gain_ref,
    pack, pack_recv, x_send, x_recv, load_sems, id_sems, x_sems,
):
    n = lax.axis_size("seq")
    s, v = lax.axis_index("seq"), lax.axis_index("vocab")
    f32, bf16, i32 = jnp.float32, jnp.bfloat16, jnp.int32
    tokens, slots = ids_ref.shape[1], routes_ref.shape[1]
    id_cap = local_ref.shape[1]
    cap = selector_ref.shape[0] // n
    blocks, block, depth = x_send.shape[1:]

    loads = [
        pltpu.make_async_copy(source, target, load_sems.at[k])
        for k, (source, target) in enumerate((
            (vision_hbm, vision_ref), (gain_hbm, gain_ref), (ids_hbm, ids_ref), (routes_hbm, routes_ref)
        ))
    ]
    for load in loads:
        load.start()
    barrier = pltpu.get_barrier_semaphore()
    for d in range(1, n):
        pl.semaphore_signal(barrier, inc=1, **at(lax.rem(s + d, n), v))
    for load in loads:
        load.wait()

    pack[...] = jnp.full(pack.shape, -1, i32)
    pack[0:1, :tokens] = ids_ref[...]
    pack[1:2, :slots] = routes_ref[...]
    pack_recv[s] = pack[...]

    group = gain_ref.shape[0]
    gain = gain_ref[...][None, :]
    for g in range(vision_ref.shape[1] // group):
        values = vision_ref[:, g * group : (g + 1) * group].astype(f32)
        center = values - jnp.mean(values, axis=-1, keepdims=True)
        spread = jnp.mean(center * center, axis=-1, keepdims=True)
        normed = (center / jnp.sqrt(spread + 1e-06) * gain).astype(bf16)
        for k in range(group // depth):
            part = normed[:, k * depth : (k + 1) * depth]
            for i in range(blocks):
                x_send[g * (group // depth) + k, i] = part[i * block : (i + 1) * block]

    pl.semaphore_wait(barrier, n - 1)

    def to_peer(source, target, sems, d, seq):
        copy = pltpu.make_async_remote_copy(
            src_ref=source,
            dst_ref=target,
            send_sem=sems.at[0, d],
            recv_sem=sems.at[1, d],
            **at(seq, v),
        )
        copy.start()
        return copy

    id_copies, x_copies = [], []
    for d in range(1, n):
        peer = lax.rem(s + d, n)
        id_copies.append(to_peer(pack, pack_recv.at[s], id_sems, d, peer))
    for d in range(1, n):
        peer = lax.rem(s + d, n)
        x_copies.append(
            to_peer(x_send.at[peer], x_slot(x_recv, s, blocks), x_sems, d, peer)
        )
    x_slot(x_recv, s, blocks)[...] = x_send[s]

    lane_t = iota((tokens, tokens), 1)
    upto = (iota((tokens, tokens), 0) <= lane_t).astype(bf16)
    before = (iota((tokens, tokens), 0) < lane_t).astype(bf16)

    own = ids_ref[...]
    home = jnp.zeros((1, tokens), i32)
    for r in range(1, n):
        home = home + (own >= r * shard_rows).astype(i32)
    home_hot = home == iota((n, tokens), 0)
    ahead = jnp.dot(home_hot.astype(bf16), before, preferred_element_type=f32)
    rank = jnp.sum(jnp.where(home_hot, ahead, 0.0), axis=0, keepdims=True)
    arrive = home.astype(f32) * id_cap + rank
    arrive = jnp.transpose(jnp.broadcast_to(arrive, (8, tokens)))[:, 0:1].astype(i32)

    owner = pack[1:2, :]
    owner_hot = owner == iota((n, LANES), 0)
    before_slot = (iota((LANES, LANES), 0) < iota((LANES, LANES), 1)).astype(bf16)
    ahead = jnp.dot(owner_hot.astype(bf16), before_slot, preferred_element_type=f32)
    rank = jnp.sum(jnp.where(owner_hot, ahead, 0.0), axis=0, keepdims=True)
    slot_of = owner * cap + rank.astype(i32)
    selector = (slot_of == iota((n * cap, LANES), 0)).astype(f32)
    selector_ref[...] = selector[:, :slots].astype(bf16)

    for copy in id_copies:
        copy.wait()
    everyone = pack_recv[...]
    all_ids, all_routes = everyone[:, 0, :tokens], everyone[:, 1, :]
    relative = all_ids - s * shard_rows
    mine = (relative >= 0) & (relative < shard_rows)
    relative = jnp.where(mine, relative, 0)
    place = jnp.dot(mine.astype(bf16), upto, preferred_element_type=f32).astype(i32) - 1
    place = jnp.where(mine, place, -1)
    high, low = relative // LANES, relative % LANES
    found_high = jnp.zeros((n, id_cap), f32)
    found_low = jnp.zeros((n, id_cap), f32)
    row_n = iota((n, id_cap), 0)
    for t in range(n):
        hot = place[t : t + 1, :] == iota((id_cap, tokens), 0)
        hot_f = hot.astype(bf16)
        pick_dims = (((1,), (1,)), ((), ()))
        part = lax.dot_general(high.astype(bf16), hot_f, pick_dims, preferred_element_type=f32)
        found_high = jnp.where(row_n == t, part, found_high)
        part = lax.dot_general(low.astype(bf16), hot_f, pick_dims, preferred_element_type=f32)
        found_low = jnp.where(row_n == t, part, found_low)
        odd = jnp.sum(jnp.where(hot, relative[t : t + 1, :] % PAIR, 0).astype(f32), axis=1, keepdims=True)
        first = t * id_cap % (pick_ref.shape[1] // PAIR)
        rows = first + iota((id_cap, pick_ref.shape[1]), 0)
        chosen = rows * PAIR + odd.astype(i32) == iota((id_cap, pick_ref.shape[1]), 1)
        pick_ref[t * id_cap : (t + 1) * id_cap, :] = chosen.astype(f32).astype(bf16)
    local_ref[...] = (found_high * LANES + found_low).astype(i32)

    counts = jnp.sum((all_routes == s).astype(f32), axis=1, keepdims=True)
    spots = image_ref.shape[1]
    sender = iota((n, LANES), 1) // cap
    count_of = jnp.sum(jnp.where(sender == iota((n, LANES), 0), counts, 0.0), axis=0, keepdims=True)
    offset_of = jnp.sum(jnp.where(sender > iota((n, LANES), 0), counts, 0.0), axis=0, keepdims=True)
    within = iota((1, LANES), 1) % cap
    start = start_ref[0]
    position = jnp.where(
        within < count_of.astype(i32), start + offset_of.astype(i32) + within, -1
    )
    image = (position == iota((tokens, LANES), 0)).astype(f32)
    image_ref[...] = image[:, :spots].astype(bf16)
    total = jnp.sum(counts).astype(i32)
    row = iota((tokens, placed_ref.shape[1]), 0)
    is_text = (row < start) | (row >= start + total)
    hot = (arrive == iota((tokens, placed_ref.shape[1]), 1)) & is_text
    placed_ref[...] = hot.astype(f32).astype(bf16)

    for copy in x_copies:
        copy.wait()
    x_ref[...] = x_recv[...]


def exchange(token_ids, routes, splice_start, vision, gain, table_rows, depth):
    n, voc = lax.axis_size("seq"), lax.axis_size("vocab")
    tokens, slots = token_ids.shape[0], routes.shape[0]
    block = n * slots // (2 * voc)
    blocks = slots // block
    id_cap, cap = 2 * tokens // n, 2 * slots // n
    i32, bf16 = jnp.int32, jnp.bfloat16
    vmem = pl.BlockSpec(memory_space=pltpu.VMEM)
    smem = pl.BlockSpec(memory_space=pltpu.SMEM)
    hbm = pl.BlockSpec(memory_space=pltpu.HBM)
    dma = pltpu.SemaphoreType.DMA
    shape = jax.ShapeDtypeStruct
    held = PAIR * min(n * id_cap, 128)

    def body(*refs):
        exchange_kernel(table_rows, *refs)

    return pl.pallas_call(
        body,
        out_shape=(
            shape((n, id_cap), i32),
            shape((n * id_cap, held), bf16),
            shape((n * cap, slots), bf16),
            shape((tokens, n * cap), bf16),
            shape((tokens, n * id_cap), bf16),
            shape((2, voc, block, depth), bf16),
        ),
        in_specs=[hbm, hbm, smem, hbm, hbm],
        out_specs=(vmem,) * 6,
        scratch_shapes=[
            pltpu.VMEM((1, tokens), i32),
            pltpu.VMEM((1, slots), i32),
            pltpu.VMEM(vision.shape, vision.dtype),
            pltpu.VMEM(gain.shape, gain.dtype),
            pltpu.VMEM((8, LANES), i32),
            pltpu.VMEM((n, 8, LANES), i32),
            pltpu.VMEM((n, blocks, block, depth), bf16),
            pltpu.VMEM((2, voc, block, depth), bf16),
            dma((4,)),
            dma((2, n)),
            dma((2, n)),
        ],
        compiler_params=pltpu.CompilerParams(
            collective_id=1, has_side_effects=True, vmem_limit_bytes=16 * 1024 * 1024
        ),
        name="exchange",
    )(
        in_hbm(token_ids[None, :]),
        in_hbm(routes.reshape(1, slots)),
        splice_start,
        in_hbm(vision),
        in_hbm(gain),
    )


def columns(width):
    return 256 if width % 256 == 0 else width


def gather_kernel(
    ids_ref, pick_ref, x_ref, table_ref, w1_hbm, out_ref, sib_ref, own_ref, w1, held, sems, w_sem
):
    groups, cap = ids_ref.shape
    span = pick_ref.shape[1]
    per = span // (PAIR * cap)
    core = lax.axis_index("seq") % 2
    load = pltpu.make_async_copy(w1_hbm, w1, w_sem)
    load.start()

    def issue(g, carry):
        for k in range(cap):
            row = pl.multiple_of(ids_ref[g, k] // PAIR * PAIR, PAIR)
            spot = pl.multiple_of((g * cap + k) * PAIR, PAIR)
            pltpu.make_async_copy(
                table_ref.at[pl.ds(row, PAIR), :], held.at[pl.ds(spot, PAIR), :], sems.at[g // per]
            ).start()
        return carry

    lax.fori_loop(0, groups, issue, 0)

    load.wait()
    mid = w1.shape[1]
    step = columns(mid)
    theirs = x_ref[1 - core].reshape(-1, w1.shape[0])
    ours = x_ref[core].reshape(-1, w1.shape[0])
    for k in range(0, mid, step):
        weight = w1[:, k : k + step]
        sib_ref[:, k : k + step] = jnp.dot(
            theirs, weight, preferred_element_type=jnp.float32
        ).astype(sib_ref.dtype)
        own_ref[:, k : k + step] = jnp.dot(ours, weight, preferred_element_type=jnp.float32)

    for g in range(groups // per):
        block = held.at[g * span : (g + 1) * span, :]
        pltpu.make_async_copy(block, block, sems.at[g]).wait()
        rows = slice(g * per * cap, (g + 1) * per * cap)
        for k in range(0, held.shape[1], 256):
            found = jnp.dot(
                pick_ref[rows, :], block[:, k : k + 256], preferred_element_type=jnp.float32
            )
            out_ref[rows, k : k + 256] = found.astype(out_ref.dtype)


def gather_rows(local_ids, pick, x, table, w1):
    groups, cap = local_ids.shape
    width = table.shape[1]
    rows, mid = x.shape[1] * x.shape[2], w1.shape[1]
    vmem = pl.BlockSpec(memory_space=pltpu.VMEM)
    hbm = pl.BlockSpec(memory_space=pltpu.HBM)
    shape = jax.ShapeDtypeStruct
    found, theirs, ours = pl.pallas_call(
        gather_kernel,
        out_shape=(
            shape((groups * cap, width), table.dtype),
            shape((rows, mid), jnp.bfloat16),
            shape((rows, mid), jnp.float32),
        ),
        in_specs=[pl.BlockSpec(memory_space=pltpu.SMEM), vmem, vmem, hbm, hbm],
        out_specs=(vmem,) * 3,
        scratch_shapes=[
            pltpu.VMEM(w1.shape, w1.dtype),
            pltpu.VMEM((groups * cap * PAIR, width), table.dtype),
            pltpu.SemaphoreType.DMA((groups * cap * PAIR // pick.shape[1],)),
            pltpu.SemaphoreType.DMA,
        ],
        compiler_params=pltpu.CompilerParams(vmem_limit_bytes=16 * 1024 * 1024),
        name="gather_rows",
    )(local_ids, pick, x, table, in_hbm(w1))
    return found.reshape(groups, cap, width), theirs, ours


def mega_kernel(
    half_send, half_own, w2_hbm, text_ref, selector_ref, image_ref, placed_ref, out_ref,
    w2, half_recv, plane_send, plane_recv, cross_recv, h_own, h_recv,
    swap_send, swap_recv, chip_sum, near_send, near_recv, far_send, far_recv,
    row_send, row_recv, text_recv, total,
    w_sem, half_sems, plane_sems, cross_sems, h_sems,
    swap_sems, near_sems, far_sems, row_sems, text_sems,
):
    n, voc = lax.axis_size("seq"), lax.axis_size("vocab")
    s, v = lax.axis_index("seq"), lax.axis_index("vocab")
    chips = n // 2
    z, c = s // 2, s % 2
    pair, side = z // 2, z % 2
    split = n // voc
    f32, bf16 = jnp.float32, jnp.bfloat16
    block = plane_recv.shape[1]
    slots = voc * block // chips
    blocks = slots // block

    load2 = pltpu.make_async_copy(w2_hbm, w2, w_sem.at[0])
    load2.start()

    barrier = pltpu.get_barrier_semaphore()
    for d in range(1, n):
        pl.semaphore_signal(barrier, inc=1, **at(lax.rem(s + d, n), v))
    for e in range(1, voc):
        pl.semaphore_signal(barrier, inc=1, **at(s, lax.rem(v + e, voc)))
    pl.semaphore_wait(barrier, n - 1 + voc - 1)

    def send(source, target, sems, spot, seq, vocab=None):
        copy = pltpu.make_async_remote_copy(
            src_ref=source,
            dst_ref=target,
            send_sem=sems.at[(0, *spot)],
            recv_sem=sems.at[(1, *spot)],
            **at(seq, v if vocab is None else vocab),
        )
        copy.start()
        return copy

    sibling = s + 1 - 2 * c
    swap = send(half_send, half_recv, half_sems, (0,), sibling)

    def text_copy(seq, source):
        return pltpu.make_async_remote_copy(
            src_ref=text_ref.at[seq],
            dst_ref=text_recv.at[source],
            send_sem=text_sems.at[0, seq],
            recv_sem=text_sems.at[1, source],
            **at(seq, v),
        )

    def send_text(turn):
        for reach in range(chips - 1, -1, -1):
            for seq in range(n):
                for other in {seq // 2 - reach, seq // 2 + reach}:
                    if 0 <= other < chips and text_turn(other, seq // 2, chips) == turn:

                        @pl.when((z == other) & (s != seq))
                        def _():
                            text_copy(seq, s).start()

    send_text(0)
    swap.wait()

    turns = sorted(range(1, voc), key=lambda e: e % 2)
    plane = {}
    for e in turns:
        peer = lax.rem(v + e, voc)
        span = pl.ds(pl.multiple_of(peer * block, block), block)
        plane_send[e] = (half_own[span, :] + half_recv[span, :].astype(f32)).astype(bf16)
        plane[e] = send(plane_send.at[e], plane_recv.at[v], plane_sems, (e,), s, peer)
    span = pl.ds(pl.multiple_of(v * block, block), block)
    plane_recv[v] = (half_own[span, :] + half_recv[span, :].astype(f32)).astype(bf16)

    inner = h_own.shape[2]

    def hidden_part(seq):
        where = pl.multiple_of(seq % split * inner, inner) if split > 1 else 0
        return plane_recv.at[seq // split, :, pl.ds(where, inner)]

    def cross_copy(seq):
        return pltpu.make_async_remote_copy(
            src_ref=hidden_part(seq),
            dst_ref=cross_recv.at[s],
            send_sem=cross_sems.at[0, seq],
            recv_sem=cross_sems.at[1, s],
            **at(seq, v),
        )

    for e in [0] + turns:
        if e:
            plane[e].wait()
        source = lax.rem(v + voc - e, voc)
        for j in range(split):
            seq = source * split + j

            @pl.when(seq != s)
            def _():
                cross_copy(seq).start()

            @pl.when(seq == s)
            def _():
                cross_recv[s] = hidden_part(seq)[...]

        if e == 0:
            text_recv[s] = text_ref[s]
            send_text(1)
    send_text(2)

    def h_place(core, vocab):
        if blocks == 1:
            return h_recv.at[core, vocab, 0]
        return h_recv.at[vocab % 2, vocab // 2, core]

    copies = []
    for core in range(2):
        for k in range(chips):
            r = 2 * k + core

            @pl.when(r != s)
            def _():
                pltpu.make_async_remote_copy(
                    src_ref=cross_recv.at[r],
                    dst_ref=cross_recv.at[r],
                    send_sem=cross_sems.at[0, r],
                    recv_sem=cross_sems.at[1, r],
                    **at(sibling, v),
                ).wait_recv()

        pre = cross_recv[core].astype(f32)
        for k in range(1, chips):
            pre = pre + cross_recv[2 * k + core].astype(f32)
        h_own[core] = (0.5 * pre * (1.0 + lax.erf(pre * math.sqrt(0.5)))).astype(bf16)
        for e in turns:
            peer = lax.rem(v + e, voc)
            copies.append(send(h_own.at[core], h_place(core, v), h_sems, (core, e), s, peer))
        h_place(core, v)[...] = h_own[core]
    send_text(3)
    load2.wait()
    for copy in copies:
        copy.wait()

    width = w2.shape[1]
    step = 512 if width % 512 == 0 else width
    chunks = [slice(k, k + step) for k in range(0, width, step)]
    depth = w2.shape[0]
    theirs = h_recv[1 - c].reshape(-1, depth)
    ours = h_recv[c].reshape(-1, depth)
    swaps = []
    for k, cols in enumerate(chunks):
        part = jnp.dot(theirs, w2[:, cols], preferred_element_type=f32)
        swap_send[:, cols] = part.astype(bf16)
        swaps.append(send(swap_send.at[:, cols], swap_recv.at[:, cols], swap_sems, (k,), sibling))
    nears = []
    for k, cols in enumerate(chunks):
        part = jnp.dot(ours, w2[:, cols], preferred_element_type=f32)
        swaps[k].wait()
        part = part + swap_recv[:, cols].astype(f32)
        chip_sum[:, :, :, cols] = part.reshape(chips // 2, 2, slots, step)
        for i in range(chips // 2):
            near_send[i, :, cols] = chip_sum[i, 1 - side, :, cols].astype(bf16)
        nears.append(send(
            near_send.at[:, :, cols], near_recv.at[:, :, cols], near_sems, (k,), s + 2 - 4 * side
        ))
    send_text(4)
    fars = []
    for k, cols in enumerate(chunks):
        nears[k].wait()
        row = []
        for i in range(1, chips // 2):
            other = lax.rem(pair + i, chips // 2)
            value = chip_sum[other, side, :, cols] + near_recv[other, :, cols].astype(f32)
            far_send[i, :, cols] = value.astype(bf16)
            row.append(send(
                far_send.at[i, :, cols], far_recv.at[i, :, cols], far_sems, (k, i),
                4 * other + 2 * side + c,
            ))
        fars.append(row)
    cap = row_send.shape[1]
    copies = []
    for k, cols in enumerate(chunks):
        value = chip_sum[pair, side, :, cols] + near_recv[pair, :, cols].astype(f32)
        for i, copy in enumerate(fars[k]):
            copy.wait()
            value = value + far_recv[i + 1, :, cols].astype(f32)
        merged = value.astype(bf16)
        outgoing = jnp.dot(selector_ref[...], merged, preferred_element_type=f32).astype(bf16)
        for t in range(n):
            row_send[t, :, cols] = outgoing[t * cap : (t + 1) * cap]
        row = []
        for d in range(1, n):
            peer = lax.rem(s + d, n)
            row.append(send(
                row_send.at[peer, :, cols], row_recv.at[s, :, cols], row_sems, (k, d), peer
            ))
        row_recv[s, :, cols] = row_send[s, :, cols]
        copies.append(row)
    for seq in range(n):

        @pl.when(seq != s)
        def _():
            text_copy(seq, s).wait_send()
            text_copy(s, seq).wait_recv()

    found = text_recv[...].reshape(-1, width)
    for cols in chunks:
        total[:, cols] = jnp.dot(
            placed_ref[...], found[:, cols], preferred_element_type=f32
        )
    for k, cols in enumerate(chunks):
        for copy in copies[k]:
            copy.wait()
        rows = row_recv[:, :, cols].astype(f32).reshape(n * cap, step).astype(bf16)
        value = total[:, cols] + jnp.dot(image_ref[...], rows, preferred_element_type=f32)
        out_ref[:, cols] = value.astype(bf16)
    for r in range(n):
        @pl.when(r != s)
        def _():
            cross_copy(r).wait_send()


TURNS = (0, 0, 2, 2, 3, 2)


def text_turn(source, target, chips):
    reach = abs(source - target)
    outer = source in (0, chips - 1)
    if reach == 0:
        return TURNS[5]
    if reach > chips // 2:
        return TURNS[0]
    if reach > chips // 4:
        return TURNS[1] if outer else TURNS[2]
    return TURNS[3] if outer or target in (0, chips - 1) else TURNS[4]


def mega(theirs, ours, w2, text, selector, image_pick, text_pick):
    n, voc = lax.axis_size("seq"), lax.axis_size("vocab")
    rows, mid = theirs.shape
    block = rows // voc
    slots = 2 * rows // n
    blocks = slots // block
    inner, width = w2.shape
    chunks = width // 512 if width % 512 == 0 else 1
    cap = selector.shape[0] // n
    bf16, f32 = jnp.bfloat16, jnp.float32
    vmem = pl.BlockSpec(memory_space=pltpu.VMEM)
    hbm = pl.BlockSpec(memory_space=pltpu.HBM)
    dma = pltpu.SemaphoreType.DMA
    return pl.pallas_call(
        mega_kernel,
        out_shape=jax.ShapeDtypeStruct((image_pick.shape[0], width), bf16),
        in_specs=[vmem, vmem, hbm, vmem, vmem, vmem, vmem],
        out_specs=vmem,
        scratch_shapes=[
            pltpu.VMEM(w2.shape, bf16),
            pltpu.VMEM(theirs.shape, bf16),
            pltpu.VMEM((voc, block, mid), bf16),
            pltpu.VMEM((voc, block, mid), bf16),
            pltpu.VMEM((n, block, inner), bf16),
            pltpu.VMEM((2, block, inner), bf16),
            pltpu.VMEM((2, n // 2, blocks, block, inner), bf16),
            pltpu.VMEM((rows, width), bf16),
            pltpu.VMEM((rows, width), bf16),
            pltpu.VMEM((n // 4, 2, slots, width), f32),
            pltpu.VMEM((n // 4, slots, width), bf16),
            pltpu.VMEM((n // 4, slots, width), bf16),
            pltpu.VMEM((n // 4, slots, width), bf16),
            pltpu.VMEM((n // 4, slots, width), bf16),
            pltpu.VMEM((n, cap, width), bf16),
            pltpu.VMEM((n, cap, width), bf16),
            pltpu.VMEM(text.shape, bf16),
            pltpu.VMEM((image_pick.shape[0], width), f32),
            dma((1,)),
            dma((2, 1)),
            dma((2, voc)),
            dma((2, n)),
            dma((2, 2, voc)),
            dma((2, chunks)),
            dma((2, chunks)),
            dma((2, chunks, n // 4)),
            dma((2, chunks, n)),
            dma((2, n)),
        ],
        compiler_params=pltpu.CompilerParams(
            collective_id=0, has_side_effects=True, vmem_limit_bytes=24 * 1024 * 1024
        ),
        name="merger",
    )(theirs, ours, in_hbm(w2), text, selector, image_pick, text_pick)


def on_device(token_ids, routes, splice_start, vision, ln_gain, table, w_fc1, w_fc2):
    local_ids, pick, selector, image_pick, text_pick, x = exchange(
        token_ids, routes, splice_start, vision, ln_gain, table.shape[0], w_fc1.shape[0]
    )
    text, theirs, ours = gather_rows(local_ids, pick, x, table, w_fc1)
    return mega(theirs, ours, w_fc2, text, selector, image_pick, text_pick)


def solution(mesh):
    in_specs = (
        P("seq"),
        P("seq", None),
        P("seq"),
        P("seq", None),
        P(),
        P("seq", "vocab"),
        P("seq", "vocab"),
        P("seq", "vocab"),
    )
    out_specs = P("seq", "vocab")
    return jax.shard_map(
        on_device, mesh=mesh, in_specs=in_specs, out_specs=out_specs, check_vma=False
    )
```

```python
import math

import jax
import jax.numpy as jnp
from jax import lax
from jax.experimental import pallas as pl
from jax.experimental.pallas import tpu as pltpu
from jax.sharding import PartitionSpec as P


PAIR = 2
LANES = 128


def at(seq, vocab):
    return dict(device_id=(seq, vocab), device_id_type=pl.DeviceIdType.MESH)


def iota(shape, dim):
    return lax.broadcasted_iota(jnp.int32, shape, dim)


def in_hbm(array):
    return pltpu.with_memory_space_constraint(array, pltpu.HBM)


def exchange_kernel(
    shard_rows, ids_hbm, routes_hbm, start_ref, vision_hbm, gain_hbm, w1_hbm,
    local_ref, pick_ref, selector_ref, image_ref, placed_ref, x_ref, w1_ref,
    ids_ref, routes_ref, vision_ref, gain_ref,
    pack, pack_recv, x_send, x_recv, load_sems, id_sems, x_sems, w_sems,
):
    n = lax.axis_size("seq")
    s, v = lax.axis_index("seq"), lax.axis_index("vocab")
    f32, bf16, i32 = jnp.float32, jnp.bfloat16, jnp.int32
    tokens, slots = ids_ref.shape[1], routes_ref.shape[1]
    id_cap = local_ref.shape[1]
    cap = selector_ref.shape[0] // n
    blocks, block, depth = x_send.shape[1:]
    z, c = s // 2, s % 2

    loads = [
        pltpu.make_async_copy(source, target, load_sems.at[k])
        for k, (source, target) in enumerate((
            (vision_hbm, vision_ref), (gain_hbm, gain_ref), (ids_hbm, ids_ref), (routes_hbm, routes_ref),
            (w1_hbm, w1_ref.at[c]),
        ))
    ]
    for load in loads:
        load.start()
    barrier = pltpu.get_barrier_semaphore()
    for d in range(1, n):
        pl.semaphore_signal(barrier, inc=1, **at(lax.rem(s + d, n), v))
    for load in loads[:4]:
        load.wait()

    pack[...] = jnp.full(pack.shape, -1, i32)
    pack[0:1, :tokens] = ids_ref[...]
    pack[1:2, :slots] = routes_ref[...]
    pack_recv[s] = pack[...]

    group = gain_ref.shape[0]
    gain = gain_ref[...][None, :]
    for g in range(vision_ref.shape[1] // group):
        values = vision_ref[:, g * group : (g + 1) * group].astype(f32)
        center = values - jnp.mean(values, axis=-1, keepdims=True)
        spread = jnp.mean(center * center, axis=-1, keepdims=True)
        normed = (center / jnp.sqrt(spread + 1e-06) * gain).astype(bf16)
        for k in range(group // depth):
            part = normed[:, k * depth : (k + 1) * depth]
            for i in range(blocks):
                x_send[g * (group // depth) + k, i] = part[i * block : (i + 1) * block]

    pl.semaphore_wait(barrier, n - 1)

    def to_peer(source, target, sems, d, seq):
        copy = pltpu.make_async_remote_copy(
            src_ref=source,
            dst_ref=target,
            send_sem=sems.at[0, d],
            recv_sem=sems.at[1, d],
            **at(seq, v),
        )
        copy.start()
        return copy

    id_copies, x_copies = [], []
    for d in range(1, n):
        peer = lax.rem(s + d, n)
        id_copies.append(to_peer(pack, pack_recv.at[s], id_sems, d, peer))
    if blocks == 1:
        for d in range(1, n // 2):
            other = lax.rem(z + d, n // 2)
            x_copies.append(
                to_peer(x_send.at[other, 0], x_recv.at[z], x_sems, d, 2 * other + c)
            )
        x_recv[z] = x_send[z, 0]
    else:
        for d in range(1, n):
            peer = lax.rem(s + d, n)
            x_copies.append(
                to_peer(x_send.at[peer // 2, peer % 2], x_recv.at[s], x_sems, d, peer)
            )
        x_recv[s] = x_send[z, c]
    share = to_peer(w1_hbm, w1_ref.at[c], w_sems, 0, s + 1 - 2 * c)

    lane_t = iota((tokens, tokens), 1)
    upto = (iota((tokens, tokens), 0) <= lane_t).astype(bf16)
    before = (iota((tokens, tokens), 0) < lane_t).astype(bf16)

    own = ids_ref[...]
    home = jnp.zeros((1, tokens), i32)
    for r in range(1, n):
        home = home + (own >= r * shard_rows).astype(i32)
    home_hot = home == iota((n, tokens), 0)
    ahead = jnp.dot(home_hot.astype(bf16), before, preferred_element_type=f32)
    rank = jnp.sum(jnp.where(home_hot, ahead, 0.0), axis=0, keepdims=True)
    arrive = home.astype(f32) * id_cap + rank
    arrive = jnp.transpose(jnp.broadcast_to(arrive, (8, tokens)))[:, 0:1].astype(i32)

    owner = pack[1:2, :]
    owner_hot = owner == iota((n, LANES), 0)
    before_slot = (iota((LANES, LANES), 0) < iota((LANES, LANES), 1)).astype(bf16)
    ahead = jnp.dot(owner_hot.astype(bf16), before_slot, preferred_element_type=f32)
    rank = jnp.sum(jnp.where(owner_hot, ahead, 0.0), axis=0, keepdims=True)
    slot_of = owner * cap + rank.astype(i32)
    selector = (slot_of == iota((n * cap, LANES), 0)).astype(f32)
    selector_ref[...] = selector[:, :slots].astype(bf16)

    for copy in id_copies:
        copy.wait()
    everyone = pack_recv[...]
    all_ids, all_routes = everyone[:, 0, :tokens], everyone[:, 1, :]
    relative = all_ids - s * shard_rows
    mine = (relative >= 0) & (relative < shard_rows)
    relative = jnp.where(mine, relative, 0)
    place = jnp.dot(mine.astype(bf16), upto, preferred_element_type=f32).astype(i32) - 1
    place = jnp.where(mine, place, -1)
    high, low = relative // LANES, relative % LANES
    found_high = jnp.zeros((n, id_cap), f32)
    found_low = jnp.zeros((n, id_cap), f32)
    row_n = iota((n, id_cap), 0)
    for t in range(n):
        hot = place[t : t + 1, :] == iota((id_cap, tokens), 0)
        hot_f = hot.astype(bf16)
        pick_dims = (((1,), (1,)), ((), ()))
        part = lax.dot_general(high.astype(bf16), hot_f, pick_dims, preferred_element_type=f32)
        found_high = jnp.where(row_n == t, part, found_high)
        part = lax.dot_general(low.astype(bf16), hot_f, pick_dims, preferred_element_type=f32)
        found_low = jnp.where(row_n == t, part, found_low)
        odd = jnp.sum(jnp.where(hot, relative[t : t + 1, :] % PAIR, 0).astype(f32), axis=1, keepdims=True)
        first = t * id_cap % (pick_ref.shape[1] // PAIR)
        rows = first + iota((id_cap, pick_ref.shape[1]), 0)
        chosen = rows * PAIR + odd.astype(i32) == iota((id_cap, pick_ref.shape[1]), 1)
        pick_ref[t * id_cap : (t + 1) * id_cap, :] = chosen.astype(f32).astype(bf16)
    local_ref[...] = (found_high * LANES + found_low).astype(i32)

    counts = jnp.sum((all_routes == s).astype(f32), axis=1, keepdims=True)
    spots = image_ref.shape[1]
    sender = iota((n, LANES), 1) // cap
    count_of = jnp.sum(jnp.where(sender == iota((n, LANES), 0), counts, 0.0), axis=0, keepdims=True)
    offset_of = jnp.sum(jnp.where(sender > iota((n, LANES), 0), counts, 0.0), axis=0, keepdims=True)
    within = iota((1, LANES), 1) % cap
    start = start_ref[0]
    position = jnp.where(
        within < count_of.astype(i32), start + offset_of.astype(i32) + within, -1
    )
    image = (position == iota((tokens, LANES), 0)).astype(f32)
    image_ref[...] = image[:, :spots].astype(bf16)
    total = jnp.sum(counts).astype(i32)
    row = iota((tokens, placed_ref.shape[1]), 0)
    is_text = (row < start) | (row >= start + total)
    hot = (arrive == iota((tokens, placed_ref.shape[1]), 1)) & is_text
    placed_ref[...] = hot.astype(f32).astype(bf16)

    for copy in x_copies:
        copy.wait()
    x_ref[...] = x_recv[...]
    loads[4].wait()
    share.wait()


def exchange(token_ids, routes, splice_start, vision, gain, table_rows, w1):
    n, voc = lax.axis_size("seq"), lax.axis_size("vocab")
    tokens, slots = token_ids.shape[0], routes.shape[0]
    block = n * slots // (2 * voc)
    blocks = slots // block
    depth = 2 * w1.shape[0]
    id_cap, cap = 2 * tokens // n, 2 * slots // n
    i32, bf16 = jnp.int32, jnp.bfloat16
    vmem = pl.BlockSpec(memory_space=pltpu.VMEM)
    smem = pl.BlockSpec(memory_space=pltpu.SMEM)
    hbm = pl.BlockSpec(memory_space=pltpu.HBM)
    dma = pltpu.SemaphoreType.DMA
    shape = jax.ShapeDtypeStruct
    held = PAIR * min(n * id_cap, 128)

    def body(*refs):
        exchange_kernel(table_rows, *refs)

    return pl.pallas_call(
        body,
        out_shape=(
            shape((n, id_cap), i32),
            shape((n * id_cap, held), bf16),
            shape((n * cap, slots), bf16),
            shape((tokens, n * cap), bf16),
            shape((tokens, n * id_cap), bf16),
            shape((voc, block, depth), bf16),
            shape((2, *w1.shape), bf16),
        ),
        in_specs=[hbm, hbm, smem, hbm, hbm, hbm],
        out_specs=(vmem,) * 7,
        scratch_shapes=[
            pltpu.VMEM((1, tokens), i32),
            pltpu.VMEM((1, slots), i32),
            pltpu.VMEM(vision.shape, vision.dtype),
            pltpu.VMEM(gain.shape, gain.dtype),
            pltpu.VMEM((8, LANES), i32),
            pltpu.VMEM((n, 8, LANES), i32),
            pltpu.VMEM((n // 2, blocks, block, depth), bf16),
            pltpu.VMEM((voc, block, depth), bf16),
            dma((5,)),
            dma((2, n)),
            dma((2, n)),
            dma((2, 1)),
        ],
        compiler_params=pltpu.CompilerParams(
            collective_id=1, has_side_effects=True, vmem_limit_bytes=16 * 1024 * 1024
        ),
        name="exchange",
    )(
        in_hbm(token_ids[None, :]),
        in_hbm(routes.reshape(1, slots)),
        splice_start,
        in_hbm(vision),
        in_hbm(gain),
        in_hbm(w1),
    )


def columns(width):
    return 256 if width % 256 == 0 else width


def gather_kernel(
    ids_ref, pick_ref, x_ref, table_ref, w1_ref, out_ref, sum_ref, held, sems
):
    groups, cap = ids_ref.shape
    span = pick_ref.shape[1]
    per = span // (PAIR * cap)

    def issue(g, carry):
        for k in range(cap):
            row = pl.multiple_of(ids_ref[g, k] // PAIR * PAIR, PAIR)
            spot = pl.multiple_of((g * cap + k) * PAIR, PAIR)
            pltpu.make_async_copy(
                table_ref.at[pl.ds(row, PAIR), :], held.at[pl.ds(spot, PAIR), :], sems.at[g // per]
            ).start()
        return carry

    lax.fori_loop(0, groups, issue, 0)

    mid = w1_ref.shape[2]
    step = columns(mid)
    voc, block, depth = x_ref.shape
    ours = x_ref[...].reshape(voc * block, depth)
    for k in range(0, mid, step):
        weight = w1_ref[:, :, k : k + step].reshape(depth, step)
        part = jnp.dot(ours, weight, preferred_element_type=jnp.float32)
        sum_ref[:, :, k : k + step] = part.astype(sum_ref.dtype).reshape(voc, block, step)

    for g in range(groups // per):
        block = held.at[g * span : (g + 1) * span, :]
        pltpu.make_async_copy(block, block, sems.at[g]).wait()
        rows = slice(g * per * cap, (g + 1) * per * cap)
        for k in range(0, held.shape[1], 256):
            found = jnp.dot(
                pick_ref[rows, :], block[:, k : k + 256], preferred_element_type=jnp.float32
            )
            out_ref[rows, k : k + 256] = found.astype(out_ref.dtype)


def gather_rows(local_ids, pick, x, table, w1):
    groups, cap = local_ids.shape
    width = table.shape[1]
    vmem = pl.BlockSpec(memory_space=pltpu.VMEM)
    hbm = pl.BlockSpec(memory_space=pltpu.HBM)
    shape = jax.ShapeDtypeStruct
    found, sums = pl.pallas_call(
        gather_kernel,
        out_shape=(
            shape((groups * cap, width), table.dtype),
            shape((*x.shape[:2], w1.shape[2]), jnp.bfloat16),
        ),
        in_specs=[pl.BlockSpec(memory_space=pltpu.SMEM), vmem, vmem, hbm, vmem],
        out_specs=(vmem,) * 2,
        scratch_shapes=[
            pltpu.VMEM((groups * cap * PAIR, width), table.dtype),
            pltpu.SemaphoreType.DMA((groups * cap * PAIR // pick.shape[1],)),
        ],
        compiler_params=pltpu.CompilerParams(vmem_limit_bytes=16 * 1024 * 1024),
        name="gather_rows",
    )(local_ids, pick, x, table, w1)
    return found.reshape(groups, cap, width), sums


def mega_kernel(
    sum_ref, w2_hbm, text_ref, selector_ref, image_ref, placed_ref, out_ref,
    w2, plane_recv, cross_recv, h_own, h_recv, halves, half_send, half_recv, chip_sum, near_send, near_recv, far_send, far_recv,
    row_send, row_recv, text_recv, total,
    w_sem, share_sems, plane_sems, cross_sems, h_sems,
    half_sems, near_sems, far_sems, row_sems, text_sems,
):
    n, voc = lax.axis_size("seq"), lax.axis_size("vocab")
    s, v = lax.axis_index("seq"), lax.axis_index("vocab")
    chips = n // 2
    z, c = s // 2, s % 2
    pair, side = z // 2, z % 2
    per = voc // chips
    f32, bf16 = jnp.float32, jnp.bfloat16
    block = plane_recv.shape[1]
    slots = voc * block // chips
    blocks = slots // block

    load2 = pltpu.make_async_copy(w2_hbm, w2.at[c], w_sem.at[0])
    load2.start()

    barrier = pltpu.get_barrier_semaphore()
    for d in range(1, n):
        pl.semaphore_signal(barrier, inc=1, **at(lax.rem(s + d, n), v))
    for e in range(1, voc):
        pl.semaphore_signal(barrier, inc=1, **at(s, lax.rem(v + e, voc)))
    pl.semaphore_wait(barrier, n - 1 + voc - 1)

    def send(source, target, sems, spot, seq, vocab=None):
        copy = pltpu.make_async_remote_copy(
            src_ref=source,
            dst_ref=target,
            send_sem=sems.at[(0, *spot)],
            recv_sem=sems.at[(1, *spot)],
            **at(seq, v if vocab is None else vocab),
        )
        copy.start()
        return copy

    sibling = s + 1 - 2 * c
    turns = sorted(range(1, voc), key=lambda e: e % 2)
    plane = {}
    for e in turns:
        peer = lax.rem(v + e, voc)
        plane[e] = send(sum_ref.at[peer], plane_recv.at[v], plane_sems, (e,), s, peer)

    def text_copy(seq, source):
        return pltpu.make_async_remote_copy(
            src_ref=text_ref.at[seq],
            dst_ref=text_recv.at[source],
            send_sem=text_sems.at[0, seq],
            recv_sem=text_sems.at[1, source],
            **at(seq, v),
        )

    def send_text(turn):
        for reach in range(chips - 1, -1, -1):
            for seq in range(n):
                for other in {seq // 2 - reach, seq // 2 + reach}:
                    if 0 <= other < chips and text_turn(other, seq // 2, chips) == turn:

                        @pl.when((z == other) & (s != seq))
                        def _():
                            text_copy(seq, s).start()

    send_text(0)
    share = send(w2_hbm, w2.at[c], share_sems, (0,), sibling)
    plane_recv[v] = sum_ref[v]

    def cross_copy(column):
        place = lax.rem(column, per)
        return pltpu.make_async_remote_copy(
            src_ref=plane_recv.at[column],
            dst_ref=cross_recv.at[z, place],
            send_sem=cross_sems.at[0, column],
            recv_sem=cross_sems.at[1, z * per + place],
            **at(2 * (column // per) + c, v),
        )

    for e in [0] + turns:
        if e:
            plane[e].wait()
        column = lax.rem(v + voc - e, voc)

        @pl.when(column // per != z)
        def _():
            cross_copy(column).start()

        @pl.when(column // per == z)
        def _():
            cross_recv[z, lax.rem(column, per)] = plane_recv[column]

        if e == 0:
            text_recv[s] = text_ref[s]
            send_text(1)
    send_text(2)

    mid = plane_recv.shape[2]
    for k in range(chips):

        @pl.when(k != z)
        def _():
            for i in range(per):
                pltpu.make_async_remote_copy(
                    src_ref=cross_recv.at[k, i],
                    dst_ref=cross_recv.at[k, i],
                    send_sem=cross_sems.at[0, k * per + i],
                    recv_sem=cross_sems.at[1, k * per + i],
                    **at(sibling, v),
                ).wait_recv()

    for i in range(per):
        pre = cross_recv[0, i].astype(f32)
        for k in range(1, chips):
            pre = pre + cross_recv[k, i].astype(f32)
        h_own[:, i * mid : (i + 1) * mid] = (
            0.5 * pre * (1.0 + lax.erf(pre * math.sqrt(0.5)))
        ).astype(bf16)
    copies = []
    for e in turns:
        peer = lax.rem(v + e, voc)
        copies.append(send(h_own, h_recv.at[v], h_sems, (e,), s, peer))
    h_recv[v] = h_own[...]
    send_text(3)
    load2.wait()
    share.wait()
    for copy in copies:
        copy.wait()

    width = w2.shape[2]
    step = 512 if width % 512 == 0 else width
    chunks = [slice(k, k + step) for k in range(0, width, step)]
    hidden = h_recv[...].reshape(voc * block, h_recv.shape[2])
    nears = []
    for k, cols in enumerate(chunks):
        weight = w2[:, :, cols].reshape(h_recv.shape[2], step)
        part = jnp.dot(hidden, weight, preferred_element_type=f32)
        chip_sum[:, :, :, cols] = part.reshape(chips // 2, 2, slots, step)
        for i in range(chips // 2):
            near_send[i, :, cols] = chip_sum[i, 1 - side, :, cols].astype(bf16)
        nears.append(send(
            near_send.at[:, :, cols], near_recv.at[:, :, cols], near_sems, (k,), s + 2 - 4 * side
        ))
    send_text(4)
    fars = []
    for k, cols in enumerate(chunks):
        nears[k].wait()
        row = []
        for i in range(1, chips // 2):
            other = lax.rem(pair + i, chips // 2)
            value = chip_sum[other, side, :, cols] + near_recv[other, :, cols].astype(f32)
            far_send[i, :, cols] = value.astype(bf16)
            row.append(send(
                far_send.at[i, :, cols], far_recv.at[i, :, cols], far_sems, (k, i),
                4 * other + 2 * side + c,
            ))
        fars.append(row)
    cap = row_send.shape[1]
    copies = []
    for k, cols in enumerate(chunks):
        value = chip_sum[pair, side, :, cols] + near_recv[pair, :, cols].astype(f32)
        for i, copy in enumerate(fars[k]):
            copy.wait()
            value = value + far_recv[i + 1, :, cols].astype(f32)
        merged = value.astype(bf16)
        if blocks == 2:
            halves[:, :, cols] = merged.reshape(2, block, step)
            half_send[:, cols] = halves[1 - c, :, cols]
            send(
                half_send.at[:, cols], half_recv.at[:, cols], half_sems, (k,), sibling
            ).wait()
            halves[1 - c, :, cols] = half_recv[:, cols]
            merged = halves[:, :, cols].reshape(slots, step)
        outgoing = jnp.dot(selector_ref[...], merged, preferred_element_type=f32).astype(bf16)
        for t in range(n):
            row_send[t, :, cols] = outgoing[t * cap : (t + 1) * cap]
        row = []
        for d in range(1, n):
            peer = lax.rem(s + d, n)
            row.append(send(
                row_send.at[peer, :, cols], row_recv.at[s, :, cols], row_sems, (k, d), peer
            ))
        row_recv[s, :, cols] = row_send[s, :, cols]
        copies.append(row)
    for seq in range(n):

        @pl.when(seq != s)
        def _():
            text_copy(seq, s).wait_send()
            text_copy(s, seq).wait_recv()

    found = text_recv[...].reshape(-1, width)
    for cols in chunks:
        total[:, cols] = jnp.dot(
            placed_ref[...], found[:, cols], preferred_element_type=f32
        )
    for k, cols in enumerate(chunks):
        for copy in copies[k]:
            copy.wait()
        rows = row_recv[:, :, cols].astype(f32).reshape(n * cap, step).astype(bf16)
        value = total[:, cols] + jnp.dot(image_ref[...], rows, preferred_element_type=f32)
        out_ref[:, cols] = value.astype(bf16)
    for column in range(voc):

        @pl.when(column // per != z)
        def _():
            cross_copy(column).wait_send()


TURNS = (0, 0, 2, 2, 3, 2)


def text_turn(source, target, chips):
    reach = abs(source - target)
    outer = source in (0, chips - 1)
    if reach == 0:
        return TURNS[5]
    if reach > chips // 2:
        return TURNS[0]
    if reach > chips // 4:
        return TURNS[1] if outer else TURNS[2]
    return TURNS[3] if outer or target in (0, chips - 1) else TURNS[4]


def mega(sums, w2, text, selector, image_pick, text_pick):
    n, voc = lax.axis_size("seq"), lax.axis_size("vocab")
    block, mid = sums.shape[1:]
    slots = 2 * voc * block // n
    blocks = slots // block
    inner, width = w2.shape
    chunks = width // 512 if width % 512 == 0 else 1
    cap = selector.shape[0] // n
    bf16, f32 = jnp.bfloat16, jnp.float32
    vmem = pl.BlockSpec(memory_space=pltpu.VMEM)
    hbm = pl.BlockSpec(memory_space=pltpu.HBM)
    dma = pltpu.SemaphoreType.DMA
    return pl.pallas_call(
        mega_kernel,
        out_shape=jax.ShapeDtypeStruct((image_pick.shape[0], width), bf16),
        in_specs=[vmem, hbm, vmem, vmem, vmem, vmem],
        out_specs=vmem,
        scratch_shapes=[
            pltpu.VMEM((2, *w2.shape), bf16),
            pltpu.VMEM((voc, block, mid), bf16),
            pltpu.VMEM((n // 2, 2 * voc // n, block, mid), bf16),
            pltpu.VMEM((block, 2 * inner), bf16),
            pltpu.VMEM((voc, block, 2 * inner), bf16),
            pltpu.VMEM((2, slots // 2, width), bf16),
            pltpu.VMEM((slots // 2, width), bf16),
            pltpu.VMEM((slots // 2, width), bf16),
            pltpu.VMEM((n // 4, 2, slots, width), f32),
            pltpu.VMEM((n // 4, slots, width), bf16),
            pltpu.VMEM((n // 4, slots, width), bf16),
            pltpu.VMEM((n // 4, slots, width), bf16),
            pltpu.VMEM((n // 4, slots, width), bf16),
            pltpu.VMEM((n, cap, width), bf16),
            pltpu.VMEM((n, cap, width), bf16),
            pltpu.VMEM(text.shape, bf16),
            pltpu.VMEM((image_pick.shape[0], width), f32),
            dma((1,)),
            dma((2, 1)),
            dma((2, voc)),
            dma((2, voc)),
            dma((2, voc)),
            dma((2, chunks)),
            dma((2, chunks)),
            dma((2, chunks, n // 4)),
            dma((2, chunks, n)),
            dma((2, n)),
        ],
        compiler_params=pltpu.CompilerParams(
            collective_id=0, has_side_effects=True, vmem_limit_bytes=24 * 1024 * 1024
        ),
        name="merger",
    )(sums, in_hbm(w2), text, selector, image_pick, text_pick)


def on_device(token_ids, routes, splice_start, vision, ln_gain, table, w_fc1, w_fc2):
    local_ids, pick, selector, image_pick, text_pick, x, w1 = exchange(
        token_ids, routes, splice_start, vision, ln_gain, table.shape[0], w_fc1
    )
    text, sums = gather_rows(local_ids, pick, x, table, w1)
    return mega(sums, w_fc2, text, selector, image_pick, text_pick)


def solution(mesh):
    in_specs = (
        P("seq"),
        P("seq", None),
        P("seq"),
        P("seq", None),
        P(),
        P("seq", "vocab"),
        P("seq", "vocab"),
        P("seq", "vocab"),
    )
    out_specs = P("seq", "vocab")
    return jax.shard_map(
        on_device, mesh=mesh, in_specs=in_specs, out_specs=out_specs, check_vma=False
    )
```

```python
import math

import jax
import jax.numpy as jnp
from jax import lax
from jax.experimental import pallas as pl
from jax.experimental.pallas import tpu as pltpu
from jax.sharding import PartitionSpec as P


PAIR = 2
LANES = 128


def at(seq, vocab):
    return dict(device_id=(seq, vocab), device_id_type=pl.DeviceIdType.MESH)


def iota(shape, dim):
    return lax.broadcasted_iota(jnp.int32, shape, dim)


def in_hbm(array):
    return pltpu.with_memory_space_constraint(array, pltpu.HBM)


def exchange_kernel(
    shard_rows, ids_hbm, routes_hbm, start_ref, vision_hbm, gain_hbm, w1_hbm,
    local_ref, pick_ref, selector_ref, image_ref, placed_ref, x_ref, w1_ref,
    ids_ref, routes_ref, vision_ref, gain_ref,
    pack, pack_recv, x_send, x_recv, load_sems, id_sems, x_sems, w_sems,
):
    n = lax.axis_size("seq")
    s, v = lax.axis_index("seq"), lax.axis_index("vocab")
    f32, bf16, i32 = jnp.float32, jnp.bfloat16, jnp.int32
    tokens, slots = ids_ref.shape[1], routes_ref.shape[1]
    id_cap = local_ref.shape[1]
    cap = selector_ref.shape[0] // n
    blocks, block, depth = x_send.shape[1:]
    z, c = s // 2, s % 2

    loads = [
        pltpu.make_async_copy(source, target, load_sems.at[k])
        for k, (source, target) in enumerate((
            (vision_hbm, vision_ref), (gain_hbm, gain_ref), (ids_hbm, ids_ref), (routes_hbm, routes_ref),
            (w1_hbm, w1_ref.at[c]),
        ))
    ]
    for load in loads:
        load.start()
    barrier = pltpu.get_barrier_semaphore()
    for d in range(1, n):
        pl.semaphore_signal(barrier, inc=1, **at(lax.rem(s + d, n), v))
    for load in loads[:4]:
        load.wait()

    pack[...] = jnp.full(pack.shape, -1, i32)
    pack[0:1, :tokens] = ids_ref[...]
    pack[1:2, :slots] = routes_ref[...]
    pack_recv[s] = pack[...]

    group = gain_ref.shape[0]
    gain = gain_ref[...][None, :]
    for g in range(vision_ref.shape[1] // group):
        values = vision_ref[:, g * group : (g + 1) * group].astype(f32)
        center = values - jnp.mean(values, axis=-1, keepdims=True)
        spread = jnp.mean(center * center, axis=-1, keepdims=True)
        normed = (center / jnp.sqrt(spread + 1e-06) * gain).astype(bf16)
        for k in range(group // depth):
            part = normed[:, k * depth : (k + 1) * depth]
            for i in range(blocks):
                x_send[g * (group // depth) + k, i] = part[i * block : (i + 1) * block]

    pl.semaphore_wait(barrier, n - 1)

    def to_peer(source, target, sems, d, seq):
        copy = pltpu.make_async_remote_copy(
            src_ref=source,
            dst_ref=target,
            send_sem=sems.at[0, d],
            recv_sem=sems.at[1, d],
            **at(seq, v),
        )
        copy.start()
        return copy

    id_copies, x_copies = [], []
    for d in range(1, n):
        peer = lax.rem(s + d, n)
        id_copies.append(to_peer(pack, pack_recv.at[s], id_sems, d, peer))
    if blocks == 1:
        for d in range(1, n // 2):
            other = lax.rem(z + d, n // 2)
            x_copies.append(
                to_peer(x_send.at[other, 0], x_recv.at[z], x_sems, d, 2 * other + c)
            )
        x_recv[z] = x_send[z, 0]
    else:
        for d in range(1, n):
            peer = lax.rem(s + d, n)
            x_copies.append(
                to_peer(x_send.at[peer // 2, peer % 2], x_recv.at[s], x_sems, d, peer)
            )
        x_recv[s] = x_send[z, c]
    share = to_peer(w1_hbm, w1_ref.at[c], w_sems, 0, s + 1 - 2 * c)

    lane_t = iota((tokens, tokens), 1)
    upto = (iota((tokens, tokens), 0) <= lane_t).astype(bf16)
    before = (iota((tokens, tokens), 0) < lane_t).astype(bf16)

    own = ids_ref[...]
    home = jnp.zeros((1, tokens), i32)
    for r in range(1, n):
        home = home + (own >= r * shard_rows).astype(i32)
    home_hot = home == iota((n, tokens), 0)
    ahead = jnp.dot(home_hot.astype(bf16), before, preferred_element_type=f32)
    rank = jnp.sum(jnp.where(home_hot, ahead, 0.0), axis=0, keepdims=True)
    arrive = home.astype(f32) * id_cap + rank
    arrive = jnp.transpose(jnp.broadcast_to(arrive, (8, tokens)))[:, 0:1].astype(i32)

    owner = pack[1:2, :]
    owner_hot = owner == iota((n, LANES), 0)
    before_slot = (iota((LANES, LANES), 0) < iota((LANES, LANES), 1)).astype(bf16)
    ahead = jnp.dot(owner_hot.astype(bf16), before_slot, preferred_element_type=f32)
    rank = jnp.sum(jnp.where(owner_hot, ahead, 0.0), axis=0, keepdims=True)
    slot_of = owner * cap + rank.astype(i32)
    selector = (slot_of == iota((n * cap, LANES), 0)).astype(f32)
    selector_ref[...] = selector[:, :slots].astype(bf16)

    for copy in id_copies:
        copy.wait()
    everyone = pack_recv[...]
    all_ids, all_routes = everyone[:, 0, :tokens], everyone[:, 1, :]
    relative = all_ids - s * shard_rows
    mine = (relative >= 0) & (relative < shard_rows)
    relative = jnp.where(mine, relative, 0)
    place = jnp.dot(mine.astype(bf16), upto, preferred_element_type=f32).astype(i32) - 1
    place = jnp.where(mine, place, -1)
    high, low = relative // LANES, relative % LANES
    found_high = jnp.zeros((n, id_cap), f32)
    found_low = jnp.zeros((n, id_cap), f32)
    row_n = iota((n, id_cap), 0)
    for t in range(n):
        hot = place[t : t + 1, :] == iota((id_cap, tokens), 0)
        hot_f = hot.astype(bf16)
        pick_dims = (((1,), (1,)), ((), ()))
        part = lax.dot_general(high.astype(bf16), hot_f, pick_dims, preferred_element_type=f32)
        found_high = jnp.where(row_n == t, part, found_high)
        part = lax.dot_general(low.astype(bf16), hot_f, pick_dims, preferred_element_type=f32)
        found_low = jnp.where(row_n == t, part, found_low)
        odd = jnp.sum(jnp.where(hot, relative[t : t + 1, :] % PAIR, 0).astype(f32), axis=1, keepdims=True)
        first = t * id_cap % (pick_ref.shape[1] // PAIR)
        rows = first + iota((id_cap, pick_ref.shape[1]), 0)
        chosen = rows * PAIR + odd.astype(i32) == iota((id_cap, pick_ref.shape[1]), 1)
        pick_ref[t * id_cap : (t + 1) * id_cap, :] = chosen.astype(f32).astype(bf16)
    local_ref[...] = (found_high * LANES + found_low).astype(i32)

    counts = jnp.sum((all_routes == s).astype(f32), axis=1, keepdims=True)
    spots = image_ref.shape[1]
    sender = iota((n, LANES), 1) // cap
    count_of = jnp.sum(jnp.where(sender == iota((n, LANES), 0), counts, 0.0), axis=0, keepdims=True)
    offset_of = jnp.sum(jnp.where(sender > iota((n, LANES), 0), counts, 0.0), axis=0, keepdims=True)
    within = iota((1, LANES), 1) % cap
    start = start_ref[0]
    position = jnp.where(
        within < count_of.astype(i32), start + offset_of.astype(i32) + within, -1
    )
    image = (position == iota((tokens, LANES), 0)).astype(f32)
    image_ref[...] = image[:, :spots].astype(bf16)
    total = jnp.sum(counts).astype(i32)
    row = iota((tokens, placed_ref.shape[1]), 0)
    is_text = (row < start) | (row >= start + total)
    hot = (arrive == iota((tokens, placed_ref.shape[1]), 1)) & is_text
    placed_ref[...] = hot.astype(f32).astype(bf16)

    for copy in x_copies:
        copy.wait()
    x_ref[...] = x_recv[...]
    loads[4].wait()
    share.wait()


def exchange(token_ids, routes, splice_start, vision, gain, table_rows, w1):
    n, voc = lax.axis_size("seq"), lax.axis_size("vocab")
    tokens, slots = token_ids.shape[0], routes.shape[0]
    block = n * slots // (2 * voc)
    blocks = slots // block
    depth = 2 * w1.shape[0]
    id_cap, cap = 2 * tokens // n, 2 * slots // n
    i32, bf16 = jnp.int32, jnp.bfloat16
    vmem = pl.BlockSpec(memory_space=pltpu.VMEM)
    smem = pl.BlockSpec(memory_space=pltpu.SMEM)
    hbm = pl.BlockSpec(memory_space=pltpu.HBM)
    dma = pltpu.SemaphoreType.DMA
    shape = jax.ShapeDtypeStruct
    held = PAIR * min(n * id_cap, 128)

    def body(*refs):
        exchange_kernel(table_rows, *refs)

    return pl.pallas_call(
        body,
        out_shape=(
            shape((n, id_cap), i32),
            shape((n * id_cap, held), bf16),
            shape((n * cap, slots), bf16),
            shape((tokens, n * cap), bf16),
            shape((tokens, n * id_cap), bf16),
            shape((voc, block, depth), bf16),
            shape((2, *w1.shape), bf16),
        ),
        in_specs=[hbm, hbm, smem, hbm, hbm, hbm],
        out_specs=(vmem,) * 7,
        scratch_shapes=[
            pltpu.VMEM((1, tokens), i32),
            pltpu.VMEM((1, slots), i32),
            pltpu.VMEM(vision.shape, vision.dtype),
            pltpu.VMEM(gain.shape, gain.dtype),
            pltpu.VMEM((8, LANES), i32),
            pltpu.VMEM((n, 8, LANES), i32),
            pltpu.VMEM((n // 2, blocks, block, depth), bf16),
            pltpu.VMEM((voc, block, depth), bf16),
            dma((5,)),
            dma((2, n)),
            dma((2, n)),
            dma((2, 1)),
        ],
        compiler_params=pltpu.CompilerParams(
            collective_id=1, has_side_effects=True, vmem_limit_bytes=16 * 1024 * 1024
        ),
        name="exchange",
    )(
        in_hbm(token_ids[None, :]),
        in_hbm(routes.reshape(1, slots)),
        splice_start,
        in_hbm(vision),
        in_hbm(gain),
        in_hbm(w1),
    )


def columns(width):
    return 256 if width % 256 == 0 else width


def gather_kernel(
    ids_ref, pick_ref, x_ref, table_ref, w1_ref, out_ref, sum_ref, held, sems
):
    groups, cap = ids_ref.shape
    span = pick_ref.shape[1]
    per = span // (PAIR * cap)

    def issue(g, carry):
        for k in range(cap):
            row = pl.multiple_of(ids_ref[g, k] // PAIR * PAIR, PAIR)
            spot = pl.multiple_of((g * cap + k) * PAIR, PAIR)
            pltpu.make_async_copy(
                table_ref.at[pl.ds(row, PAIR), :], held.at[pl.ds(spot, PAIR), :], sems.at[g // per]
            ).start()
        return carry

    lax.fori_loop(0, groups, issue, 0)

    mid = w1_ref.shape[2]
    step = columns(mid)
    voc, block, depth = x_ref.shape
    ours = x_ref[...].reshape(voc * block, depth)
    for k in range(0, mid, step):
        weight = w1_ref[:, :, k : k + step].reshape(depth, step)
        part = jnp.dot(ours, weight, preferred_element_type=jnp.float32)
        sum_ref[:, :, k : k + step] = part.astype(sum_ref.dtype).reshape(voc, block, step)

    for g in range(groups // per):
        block = held.at[g * span : (g + 1) * span, :]
        pltpu.make_async_copy(block, block, sems.at[g]).wait()
        rows = slice(g * per * cap, (g + 1) * per * cap)
        for k in range(0, held.shape[1], 256):
            found = jnp.dot(
                pick_ref[rows, :], block[:, k : k + 256], preferred_element_type=jnp.float32
            )
            out_ref[rows, k : k + 256] = found.astype(out_ref.dtype)


def gather_rows(local_ids, pick, x, table, w1):
    groups, cap = local_ids.shape
    width = table.shape[1]
    vmem = pl.BlockSpec(memory_space=pltpu.VMEM)
    hbm = pl.BlockSpec(memory_space=pltpu.HBM)
    shape = jax.ShapeDtypeStruct
    found, sums = pl.pallas_call(
        gather_kernel,
        out_shape=(
            shape((groups * cap, width), table.dtype),
            shape((*x.shape[:2], w1.shape[2]), jnp.bfloat16),
        ),
        in_specs=[pl.BlockSpec(memory_space=pltpu.SMEM), vmem, vmem, hbm, vmem],
        out_specs=(vmem,) * 2,
        scratch_shapes=[
            pltpu.VMEM((groups * cap * PAIR, width), table.dtype),
            pltpu.SemaphoreType.DMA((groups * cap * PAIR // pick.shape[1],)),
        ],
        compiler_params=pltpu.CompilerParams(vmem_limit_bytes=16 * 1024 * 1024),
        name="gather_rows",
    )(local_ids, pick, x, table, w1)
    return found.reshape(groups, cap, width), sums


def mega_kernel(
    sum_ref, w2_hbm, text_ref, selector_ref, image_ref, placed_ref, out_ref,
    w2, plane_recv, cross_recv, h_own, h_recv, halves, half_send, half_recv, chip_sum, near_send, near_recv, far_send, far_recv,
    row_send, row_recv, text_recv, total,
    w_sem, share_sems, plane_sems, cross_sems, h_sems,
    half_sems, near_sems, far_sems, row_sems, text_sems,
):
    n, voc = lax.axis_size("seq"), lax.axis_size("vocab")
    s, v = lax.axis_index("seq"), lax.axis_index("vocab")
    chips = n // 2
    z, c = s // 2, s % 2
    pair, side = z // 2, z % 2
    per = voc // chips
    f32, bf16 = jnp.float32, jnp.bfloat16
    block = plane_recv.shape[1]
    slots = voc * block // chips
    blocks = slots // block

    load2 = pltpu.make_async_copy(w2_hbm, w2.at[c], w_sem.at[0])
    load2.start()

    barrier = pltpu.get_barrier_semaphore()
    for d in range(1, n):
        pl.semaphore_signal(barrier, inc=1, **at(lax.rem(s + d, n), v))
    for e in range(1, voc):
        pl.semaphore_signal(barrier, inc=1, **at(s, lax.rem(v + e, voc)))
    pl.semaphore_wait(barrier, n - 1 + voc - 1)

    def send(source, target, sems, spot, seq, vocab=None):
        copy = pltpu.make_async_remote_copy(
            src_ref=source,
            dst_ref=target,
            send_sem=sems.at[(0, *spot)],
            recv_sem=sems.at[(1, *spot)],
            **at(seq, v if vocab is None else vocab),
        )
        copy.start()
        return copy

    sibling = s + 1 - 2 * c
    turns = sorted(range(1, voc), key=lambda e: e % 2)
    plane = {}
    for e in turns:
        peer = lax.rem(v + e, voc)
        plane[e] = send(sum_ref.at[peer], plane_recv.at[v], plane_sems, (e,), s, peer)

    def text_copy(seq, source):
        return pltpu.make_async_remote_copy(
            src_ref=text_ref.at[seq],
            dst_ref=text_recv.at[source],
            send_sem=text_sems.at[0, seq],
            recv_sem=text_sems.at[1, source],
            **at(seq, v),
        )

    def send_text(turn):
        for reach in range(chips - 1, -1, -1):
            for seq in range(n):
                for other in {seq // 2 - reach, seq // 2 + reach}:
                    if 0 <= other < chips and text_turn(other, seq // 2, seq % 2, chips) == turn:

                        @pl.when((z == other) & (s != seq))
                        def _():
                            text_copy(seq, s).start()

    send_text(0)
    share = send(w2_hbm, w2.at[c], share_sems, (0,), sibling)
    plane_recv[v] = sum_ref[v]

    def cross_copy(column):
        place = lax.rem(column, per)
        return pltpu.make_async_remote_copy(
            src_ref=plane_recv.at[column],
            dst_ref=cross_recv.at[z, place],
            send_sem=cross_sems.at[0, column],
            recv_sem=cross_sems.at[1, z * per + place],
            **at(2 * (column // per) + c, v),
        )

    for e in [0] + turns:
        if e:
            plane[e].wait()
        column = lax.rem(v + voc - e, voc)

        @pl.when(column // per != z)
        def _():
            cross_copy(column).start()

        @pl.when(column // per == z)
        def _():
            cross_recv[z, lax.rem(column, per)] = plane_recv[column]

        if e == 0:
            text_recv[s] = text_ref[s]
            send_text(1)
    send_text(2)

    mid = plane_recv.shape[2]
    for k in range(chips):

        @pl.when(k != z)
        def _():
            for i in range(per):
                pltpu.make_async_remote_copy(
                    src_ref=cross_recv.at[k, i],
                    dst_ref=cross_recv.at[k, i],
                    send_sem=cross_sems.at[0, k * per + i],
                    recv_sem=cross_sems.at[1, k * per + i],
                    **at(sibling, v),
                ).wait_recv()

    for i in range(per):
        pre = cross_recv[0, i].astype(f32)
        for k in range(1, chips):
            pre = pre + cross_recv[k, i].astype(f32)
        h_own[:, i * mid : (i + 1) * mid] = (
            0.5 * pre * (1.0 + lax.erf(pre * math.sqrt(0.5)))
        ).astype(bf16)
    copies = []
    for e in turns:
        peer = lax.rem(v + e, voc)
        copies.append(send(h_own, h_recv.at[v], h_sems, (e,), s, peer))
    h_recv[v] = h_own[...]
    send_text(3)
    load2.wait()
    share.wait()
    for copy in copies:
        copy.wait()

    width = w2.shape[2]
    step = 512 if width % 512 == 0 else width
    chunks = [slice(k, k + step) for k in range(0, width, step)]
    hidden = h_recv[...].reshape(voc * block, h_recv.shape[2])
    nears = []
    for k, cols in enumerate(chunks):
        weight = w2[:, :, cols].reshape(h_recv.shape[2], step)
        part = jnp.dot(hidden, weight, preferred_element_type=f32)
        chip_sum[:, :, :, cols] = part.reshape(chips // 2, 2, slots, step)
        for i in range(chips // 2):
            near_send[i, :, cols] = chip_sum[i, 1 - side, :, cols].astype(bf16)
        nears.append(send(
            near_send.at[:, :, cols], near_recv.at[:, :, cols], near_sems, (k,), s + 2 - 4 * side
        ))
    send_text(4)
    fars = []
    for k, cols in enumerate(chunks):
        nears[k].wait()
        row = []
        for i in range(1, chips // 2):
            other = lax.rem(pair + i, chips // 2)
            value = chip_sum[other, side, :, cols] + near_recv[other, :, cols].astype(f32)
            far_send[i, :, cols] = value.astype(bf16)
            row.append(send(
                far_send.at[i, :, cols], far_recv.at[i, :, cols], far_sems, (k, i),
                4 * other + 2 * side + c,
            ))
        fars.append(row)
    cap = row_send.shape[1]
    copies = []
    for k, cols in enumerate(chunks):
        value = chip_sum[pair, side, :, cols] + near_recv[pair, :, cols].astype(f32)
        for i, copy in enumerate(fars[k]):
            copy.wait()
            value = value + far_recv[i + 1, :, cols].astype(f32)
        merged = value.astype(bf16)
        if blocks == 2:
            halves[:, :, cols] = merged.reshape(2, block, step)
            half_send[:, cols] = halves[1 - c, :, cols]
            send(
                half_send.at[:, cols], half_recv.at[:, cols], half_sems, (k,), sibling
            ).wait()
            halves[1 - c, :, cols] = half_recv[:, cols]
            merged = halves[:, :, cols].reshape(slots, step)
        outgoing = jnp.dot(selector_ref[...], merged, preferred_element_type=f32).astype(bf16)
        for t in range(n):
            row_send[t, :, cols] = outgoing[t * cap : (t + 1) * cap]
        row = []
        for d in range(1, n):
            peer = lax.rem(s + d, n)
            row.append(send(
                row_send.at[peer, :, cols], row_recv.at[s, :, cols], row_sems, (k, d), peer
            ))
        row_recv[s, :, cols] = row_send[s, :, cols]
        copies.append(row)
    for seq in range(n):

        @pl.when(seq != s)
        def _():
            text_copy(seq, s).wait_send()
            text_copy(s, seq).wait_recv()

    found = text_recv[...].reshape(-1, width)
    for cols in chunks:
        total[:, cols] = jnp.dot(
            placed_ref[...], found[:, cols], preferred_element_type=f32
        )
    for k, cols in enumerate(chunks):
        for copy in copies[k]:
            copy.wait()
        rows = row_recv[:, :, cols].astype(f32).reshape(n * cap, step).astype(bf16)
        value = total[:, cols] + jnp.dot(image_ref[...], rows, preferred_element_type=f32)
        out_ref[:, cols] = value.astype(bf16)
    for column in range(voc):

        @pl.when(column // per != z)
        def _():
            cross_copy(column).wait_send()


TURNS = ((0, 0, 2, 2, 3, 2), (0, 2, 2, 2, 2, 2))


def text_turn(source, target, core, chips):
    turns = TURNS[core]
    reach = abs(source - target)
    outer = source in (0, chips - 1)
    if reach == 0:
        return turns[5]
    if reach > chips // 2:
        return turns[0]
    if reach > chips // 4:
        return turns[1] if outer else turns[2]
    return turns[3] if outer or target in (0, chips - 1) else turns[4]


def mega(sums, w2, text, selector, image_pick, text_pick):
    n, voc = lax.axis_size("seq"), lax.axis_size("vocab")
    block, mid = sums.shape[1:]
    slots = 2 * voc * block // n
    blocks = slots // block
    inner, width = w2.shape
    chunks = width // 512 if width % 512 == 0 else 1
    cap = selector.shape[0] // n
    bf16, f32 = jnp.bfloat16, jnp.float32
    vmem = pl.BlockSpec(memory_space=pltpu.VMEM)
    hbm = pl.BlockSpec(memory_space=pltpu.HBM)
    dma = pltpu.SemaphoreType.DMA
    return pl.pallas_call(
        mega_kernel,
        out_shape=jax.ShapeDtypeStruct((image_pick.shape[0], width), bf16),
        in_specs=[vmem, hbm, vmem, vmem, vmem, vmem],
        out_specs=vmem,
        scratch_shapes=[
            pltpu.VMEM((2, *w2.shape), bf16),
            pltpu.VMEM((voc, block, mid), bf16),
            pltpu.VMEM((n // 2, 2 * voc // n, block, mid), bf16),
            pltpu.VMEM((block, 2 * inner), bf16),
            pltpu.VMEM((voc, block, 2 * inner), bf16),
            pltpu.VMEM((2, slots // 2, width), bf16),
            pltpu.VMEM((slots // 2, width), bf16),
            pltpu.VMEM((slots // 2, width), bf16),
            pltpu.VMEM((n // 4, 2, slots, width), f32),
            pltpu.VMEM((n // 4, slots, width), bf16),
            pltpu.VMEM((n // 4, slots, width), bf16),
            pltpu.VMEM((n // 4, slots, width), bf16),
            pltpu.VMEM((n // 4, slots, width), bf16),
            pltpu.VMEM((n, cap, width), bf16),
            pltpu.VMEM((n, cap, width), bf16),
            pltpu.VMEM(text.shape, bf16),
            pltpu.VMEM((image_pick.shape[0], width), f32),
            dma((1,)),
            dma((2, 1)),
            dma((2, voc)),
            dma((2, voc)),
            dma((2, voc)),
            dma((2, chunks)),
            dma((2, chunks)),
            dma((2, chunks, n // 4)),
            dma((2, chunks, n)),
            dma((2, n)),
        ],
        compiler_params=pltpu.CompilerParams(
            collective_id=0, has_side_effects=True, vmem_limit_bytes=24 * 1024 * 1024
        ),
        name="merger",
    )(sums, in_hbm(w2), text, selector, image_pick, text_pick)


def on_device(token_ids, routes, splice_start, vision, ln_gain, table, w_fc1, w_fc2):
    local_ids, pick, selector, image_pick, text_pick, x, w1 = exchange(
        token_ids, routes, splice_start, vision, ln_gain, table.shape[0], w_fc1
    )
    text, sums = gather_rows(local_ids, pick, x, table, w1)
    return mega(sums, w_fc2, text, selector, image_pick, text_pick)


def solution(mesh):
    in_specs = (
        P("seq"),
        P("seq", None),
        P("seq"),
        P("seq", None),
        P(),
        P("seq", "vocab"),
        P("seq", "vocab"),
        P("seq", "vocab"),
    )
    out_specs = P("seq", "vocab")
    return jax.shard_map(
        on_device, mesh=mesh, in_specs=in_specs, out_specs=out_specs, check_vma=False
    )
```
